64 devices in a mesh: dp: 4 (over x, y), tp: 16 (over z, core).
Axes of the slice: x: 2, y: 2, z: 8, core: 2. Of those that a mesh axis runs over, the one named last changes fastest.
The devices are a block of a 4x4x8 slice.
Arguments:
- token_ids: int32 [4, 2048], P('dp'), parts along dimension 0
- word_table: bfloat16 [50432, 6144], P('tp')
- pos_table: bfloat16 [2048, 6144], replicated
- ln_gain: float32 [6144], replicated
- ln_bias: float32 [6144], replicated
- w_qkv: bfloat16 [6144, 3, 64, 96], P(None, None, 'tp')
- b_qkv: float32 [3, 64, 96], P(None, 'tp')
- w_out: bfloat16 [64, 96, 6144], P('tp')
- b_out: float32 [6144], replicated
Outputs:
- output 1: bfloat16 [4, 2048, 6144], P('dp', 'tp'), parts along dimension 0
- output 2: bfloat16 [4, 2048, 6144], P('dp', 'tp'), parts along dimension 0
There are 4 independent parts. The reference program is written for one: setup_inputs(seed, part) draws one part's arguments, and reference() takes and returns one part's arrays. A program takes and returns all parts, laid end to end along the dimension named above; an argument that names none is the same for every part.
All inputs are finite; a program needn't handle non-finite values.
Results may differ from the reference program's by a relative error of at most 0.00753435.
Values are sent between devices in bfloat16 or wider.
A program may use at most 768 MiB of HBM per device.

```python
import math
import jax
import jax.numpy as jnp
from jax import lax

VOCAB_SIZE = 50432
MODEL_DIM = 6144
NUM_HEADS = 64
HEAD_DIM = 96
SEQ_LEN = 2048
GROUP_BATCH = 1
OCTAVES = math.ceil(math.log2(VOCAB_SIZE))
LN_EPS = 1e-5


def draw_token_ids(key):
    key_octave, key_rank, key_order = jax.random.split(key, 3)
    id_shape = (GROUP_BATCH, SEQ_LEN)
    octave = jax.random.randint(key_octave, id_shape, 0, OCTAVES + 1)
    rank_span = jnp.minimum(jnp.left_shift(jnp.ones(id_shape, jnp.int32), octave), VOCAB_SIZE)
    rank = jax.random.randint(key_rank, id_shape, 0, rank_span)
    vocab_order = jax.random.permutation(key_order, VOCAB_SIZE)
    return jnp.take(vocab_order, rank).astype(jnp.int32)


def setup_inputs(seed: int = 0, part: int = 0) -> dict:
    base_key = jax.random.key(seed)
    part_key = jax.random.fold_in(base_key, part)
    keys = jax.random.split(base_key, 8)
    token_ids = draw_token_ids(part_key)
    word_table = (0.8 * jax.random.normal(keys[0], (VOCAB_SIZE, MODEL_DIM), jnp.float32)).astype(jnp.bfloat16)
    pos_table = (0.6 * jax.random.normal(keys[1], (SEQ_LEN, MODEL_DIM), jnp.float32)).astype(jnp.bfloat16)
    ln_gain = 1.0 + 0.2 * jax.random.normal(keys[2], (MODEL_DIM,), jnp.float32)
    ln_bias = 0.2 * jax.random.normal(keys[3], (MODEL_DIM,), jnp.float32)
    qkv_scale = jnp.array([3.0 ** 0.5, 3.0 ** 0.5, 1.0], jnp.float32) * MODEL_DIM ** -0.5
    w_qkv = (jax.random.normal(keys[4], (MODEL_DIM, 3, NUM_HEADS, HEAD_DIM), jnp.float32) * qkv_scale[None, :, None, None]).astype(jnp.bfloat16)
    b_qkv = 0.3 * jax.random.normal(keys[5], (3, NUM_HEADS, HEAD_DIM), jnp.float32)
    w_out = (jax.random.normal(keys[6], (NUM_HEADS, HEAD_DIM, MODEL_DIM), jnp.float32) * (NUM_HEADS * HEAD_DIM) ** -0.5).astype(jnp.bfloat16)
    b_out = 0.3 * jax.random.normal(keys[7], (MODEL_DIM,), jnp.float32)
    return {"token_ids": token_ids, "word_table": word_table, "pos_table": pos_table, "ln_gain": ln_gain, "ln_bias": ln_bias, "w_qkv": w_qkv, "b_qkv": b_qkv, "w_out": w_out, "b_out": b_out}


def layer_norm(values, gain, bias):
    feat_mean = jnp.mean(values, axis=-1, keepdims=True)
    centered = values - feat_mean
    feat_variance = jnp.mean(centered * centered, axis=-1, keepdims=True)
    return centered * lax.rsqrt(feat_variance + LN_EPS) * gain + bias


def reference(token_ids, word_table, pos_table, ln_gain, ln_bias, w_qkv, b_qkv, w_out, b_out):
    table_rows = jnp.take(word_table, token_ids, axis=0).astype(jnp.float32)
    embed = (table_rows + pos_table.astype(jnp.float32)[None]).astype(jnp.bfloat16)
    normed = layer_norm(embed.astype(jnp.float32), ln_gain, ln_bias).astype(jnp.bfloat16)
    inner_width = NUM_HEADS * HEAD_DIM
    projected = jnp.dot(normed.reshape(GROUP_BATCH * SEQ_LEN, MODEL_DIM), w_qkv.reshape(MODEL_DIM, 3 * inner_width), preferred_element_type=jnp.float32)
    projected = (projected.reshape(GROUP_BATCH, SEQ_LEN, 3, NUM_HEADS, HEAD_DIM) + b_qkv).astype(jnp.bfloat16)
    heads_first = jnp.transpose(projected, (2, 0, 3, 1, 4)).reshape(3, GROUP_BATCH * NUM_HEADS, SEQ_LEN, HEAD_DIM)
    positions = jnp.arange(SEQ_LEN)
    causal_mask = positions[:, None] >= positions[None, :]

    def one_head(operands):
        query_h, key_h, value_h = operands
        attn_scores = jnp.dot(query_h, key_h.T, preferred_element_type=jnp.float32) * HEAD_DIM ** -0.5
        attn_scores = jnp.where(causal_mask, attn_scores, -jnp.inf)
        attn_probs = jax.nn.softmax(attn_scores, axis=-1).astype(jnp.bfloat16)
        return jnp.dot(attn_probs, value_h, preferred_element_type=jnp.float32).astype(jnp.bfloat16)

    context = lax.map(one_head, (heads_first[0], heads_first[1], heads_first[2]))
    context = context.reshape(GROUP_BATCH, NUM_HEADS, SEQ_LEN, HEAD_DIM)
    attn_out = jnp.einsum("bhse,hed->bsd", context.astype(jnp.float32), w_out.astype(jnp.float32))
    resid_out = (embed.astype(jnp.float32) + attn_out + b_out).astype(jnp.bfloat16)
    return resid_out, embed
```

```python
import functools

import jax
import jax.numpy as jnp
from jax import lax
from jax.experimental import pallas as pl
from jax.experimental.pallas import tpu as pltpu
from jax.sharding import PartitionSpec as P

LN_EPS = 1e-5
MESH = pl.DeviceIdType.MESH
BF16 = jnp.bfloat16
F32 = jnp.float32
VMEM_LIMIT = 67043328


def layer_norm(values, gain, bias):
    feat_mean = jnp.mean(values, axis=-1, keepdims=True)
    centered = values - feat_mean
    feat_variance = jnp.mean(centered * centered, axis=-1, keepdims=True)
    return centered * lax.rsqrt(feat_variance + LN_EPS) * gain + bias


ROWS = 16
FETCHES = 16
NONE = -(2**30)


def gather_kernel(block_len, shard_rows, ids_ref, column_ref, table_ref, out_ref, found, count, stamp, fetched, sems):
    j = pl.program_id(0)
    n_blocks = pl.num_programs(0)
    n_groups = shard_rows // ROWS

    def scan(block):
        base = lax.rem(block, 2) * (2 * block_len)

        def one(q, total):
            local_id = ids_ref[block * block_len + q]
            mine = (local_id >= 0) & (local_id < shard_rows)
            group = jnp.where(mine, lax.div(local_id, ROWS), n_groups)
            fresh = mine & (stamp[group] != block)
            stamp[group] = block
            found[base + total] = group
            return total + jnp.where(fresh, 1, 0)

        count[lax.rem(block, 2)] = lax.fori_loop(0, block_len, one, 0, unroll=8)

    def copy_of(block, chunk, k, slot):
        group = found[lax.rem(block, 2) * (2 * block_len) + chunk * FETCHES + k]
        return pltpu.make_async_copy(
            table_ref.at[pl.ds(pl.multiple_of(group * ROWS, ROWS), ROWS), :],
            fetched.at[slot, pl.ds(pl.multiple_of(k * ROWS, ROWS), ROWS), :],
            sems.at[slot, k],
        )

    def in_chunk(block, chunk):
        return jnp.minimum(count[lax.rem(block, 2)] - chunk * FETCHES, FETCHES)

    def start(block, chunk, slot):
        def one(k, carry):
            copy_of(block, chunk, k, slot).start()
            return carry

        lax.fori_loop(0, in_chunk(block, chunk), one, 0)

    def wait(block, chunk, slot):
        def one(k, carry):
            copy_of(block, chunk, k, slot).wait()
            return carry

        lax.fori_loop(0, in_chunk(block, chunk), one, 0)

    def selector(block, chunk):
        columns = lax.broadcasted_iota(jnp.int32, (1, FETCHES * ROWS), 1)
        base = lax.rem(block, 2) * (2 * block_len) + chunk * FETCHES
        held = in_chunk(block, chunk)
        first = jnp.full((1, FETCHES * ROWS), NONE, jnp.int32)
        for k in range(FETCHES):
            first = jnp.where(lax.div(columns, ROWS) == k, jnp.where(k < held, found[base + k] * ROWS, NONE), first)
        return jnp.where(column_ref[...] == first + lax.rem(columns, ROWS), 1.0, 0.0).astype(BF16)

    @pl.when(j == 0)
    def _():
        fetched[...] = jnp.zeros_like(fetched)

        def clear(g, carry):
            stamp[g] = -1
            return carry

        lax.fori_loop(0, n_groups + 1, clear, 0)
        scan(0)
        start(0, 0, 0)

    @pl.when(j + 1 < n_blocks)
    def _():
        scan(j + 1)
        start(j + 1, 0, lax.rem(j + 1, 2))

    slot = lax.rem(j, 2)
    wait(j, 0, slot)
    out_ref[...] = jnp.dot(selector(j, 0), fetched[slot], preferred_element_type=F32).astype(BF16)

    def more(chunk, carry):
        start(j, chunk, slot)
        wait(j, chunk, slot)
        out_ref[...] += jnp.dot(selector(j, chunk), fetched[slot], preferred_element_type=F32).astype(BF16)
        return carry

    lax.fori_loop(1, lax.div(count[slot] + (FETCHES - 1), FETCHES), more, 0)


def gather_rows(local_ids, table, block_len):
    (n_ids,), (shard_rows, width) = local_ids.shape, table.shape
    return pl.pallas_call(
        functools.partial(gather_kernel, block_len, shard_rows),
        grid=(n_ids // block_len,),
        out_shape=jax.ShapeDtypeStruct((n_ids, width), BF16),
        in_specs=[
            pl.BlockSpec(memory_space=pltpu.SMEM),
            pl.BlockSpec((block_len, 1), lambda j: (j, 0)),
            pl.BlockSpec(memory_space=pl.ANY),
        ],
        out_specs=pl.BlockSpec((block_len, width), lambda j: (j, 0)),
        scratch_shapes=[
            pltpu.SMEM((4 * block_len,), jnp.int32),
            pltpu.SMEM((2,), jnp.int32),
            pltpu.SMEM((shard_rows // ROWS + 1,), jnp.int32),
            pltpu.VMEM((2, FETCHES * ROWS, width), BF16),
            pltpu.SemaphoreType.DMA((2, FETCHES)),
        ],
        compiler_params=pltpu.CompilerParams(vmem_limit_bytes=40 * 2**20),
        name="gather_rows",
    )(local_ids, local_ids.reshape(n_ids, 1), table)


class Ring:
    def __init__(self, n):
        self.chips = n // 2
        self.me = lax.axis_index("tp")
        self.odd = lax.rem(self.me, 2)
        self.chip = lax.div(self.me, 2)
        self.way = 2 * self.odd - 1
        self.near = self.me - self.way
        self.far = lax.rem(self.me + self.way + n, n)

    def near_block(self, k):
        return 2 * lax.rem(self.chip - self.way * k + 2 * self.chips, self.chips) + self.odd

    def far_block(self, k):
        return 2 * lax.rem(self.chip + self.way * k + 2 * self.chips, self.chips) + 1 - self.odd

    def barrier(self):
        sem = pltpu.get_barrier_semaphore()
        for device in (self.near, self.far):
            pl.semaphore_signal(sem, inc=1, device_id={"tp": device}, device_id_type=MESH)
        pl.semaphore_wait(sem, 2)


def remote(src, dst, send_sem, recv_sem, device):
    return pltpu.make_async_remote_copy(
        src_ref=src, dst_ref=dst, send_sem=send_sem, recv_sem=recv_sem, device_id={"tp": device}, device_id_type=MESH
    )


def ring_sum_kernel(n, part_ref, out_ref, own_n, own_f, buf_n, buf_f, own_sem, send_f, send_n, recv_f, recv_n):
    ring = Ring(n)

    def load_n(t):
        return pltpu.make_async_copy(part_ref.at[ring.near_block(lax.div(t, 2) + 1), lax.rem(t, 2)], own_n.at[t], own_sem.at[0, t])

    def load_f(t):
        return pltpu.make_async_copy(part_ref.at[ring.far_block(lax.div(t, 2) + 1), lax.rem(t, 2)], own_f.at[t], own_sem.at[1, t])

    def start_loads(t, carry):
        load_f(t).start()
        load_n(t).start()
        return carry

    lax.fori_loop(0, n, start_loads, 0)
    ring.barrier()

    def to_far(src, t):
        return remote(src, buf_f.at[t], send_f.at[t], recv_f.at[t], ring.far)

    def to_near(src, t):
        return remote(src, buf_n.at[t], send_n.at[t], recv_n.at[t], ring.near)

    def pass_far_on(t):
        to_far(buf_f.at[t], t).wait_recv()
        load_f(t + 2).wait()
        buf_f[t] = buf_f[t] + own_f[t + 2]
        to_near(buf_f.at[t], t + 2).start()

    def take_near(t):
        to_near(buf_n.at[t], t).wait_recv()
        load_n(t).wait()

    def pass_near_on(t):
        take_near(t)
        buf_n[t] = buf_n[t] + own_n[t]
        to_far(buf_n.at[t], t).start()

    def finish_near(t):
        take_near(t)
        out_ref[t % 2] = buf_n[t] + own_n[t]

    for t in range(2):
        load_f(t).wait()
        to_near(own_f.at[t], t).start()
    for t in range(2):
        pass_near_on(t)

    def step(t, carry):
        pass_far_on(t)
        pass_near_on(t + 2)
        return carry

    lax.fori_loop(0, n - 4, step, 0)
    for t in (n - 4, n - 3):
        pass_far_on(t)
        finish_near(t + 2)

    def finish(t, carry):
        to_near(own_f.at[t], t).wait_send()
        return carry

    lax.fori_loop(0, n, finish, 0)

    def finish_far(t, carry):
        to_far(buf_n.at[t], t).wait_send()
        return carry

    lax.fori_loop(0, n - 2, finish_far, 0)


def ring_sum(partial_rows, n):
    _, _, half, width = partial_rows.shape
    dma = pltpu.SemaphoreType.DMA
    return pl.pallas_call(
        functools.partial(ring_sum_kernel, n),
        out_shape=jax.ShapeDtypeStruct((2, half, width), BF16),
        in_specs=[pl.BlockSpec(memory_space=pl.ANY)],
        out_specs=pl.BlockSpec(memory_space=pltpu.VMEM),
        scratch_shapes=[
            pltpu.VMEM((n, half, width), BF16),
            pltpu.VMEM((n, half, width), BF16),
            pltpu.VMEM((n, half, width), BF16),
            pltpu.VMEM((n - 2, half, width), BF16),
            dma((2, n)), dma((n - 2,)), dma((n,)), dma((n - 2,)), dma((n,)),
        ],
        compiler_params=pltpu.CompilerParams(collective_id=1, has_side_effects=True, vmem_limit_bytes=VMEM_LIMIT),
        name="ring_sum",
    )(partial_rows)


def ring_qkv_kernel(n, own_ref, w_hbm, bias_ref, out_ref, w_ref, buf_n, buf_f, w_sem, send_f, send_n, recv_f, recv_n):
    ring = Ring(n)
    half, width = own_ref.shape[1:]
    n_parts, part_width = w_ref.shape[:2]
    load_w = pltpu.make_async_copy(w_hbm, w_ref, w_sem.at[0])
    load_w.start()
    ring.barrier()

    def to_far(src, t):
        return remote(src, buf_f.at[t], send_f.at[t], recv_f.at[t], ring.far)

    def to_near(src, t):
        return remote(src, buf_n.at[t], send_n.at[t], recv_n.at[t], ring.near)

    def multiply(rows, block, low, high):
        def one(c, carry):
            product = lax.dot_general(
                rows[...].reshape(2 * half, width), w_ref[c], (((1,), (1,)), ((), ())), preferred_element_type=F32
            )
            product = (product + bias_ref[c]).astype(BF16)
            out_ref[c, block, :, :, :part_width] = product.reshape(2, half, part_width)
            return carry

        lax.fori_loop(low, high, one, 0)

    for t in range(2):
        to_far(own_ref.at[t], t).start()
    for t in range(2):
        to_near(own_ref.at[t], t).start()
    out_ref[...] = jnp.zeros_like(out_ref)
    load_w.wait()
    multiply(own_ref, ring.me, 0, n_parts)
    for t in range(2):
        to_near(buf_n.at[t], t).wait_recv()
    mid = n_parts // 2

    def step(k, carry):
        near_owner = jnp.where(k == 0, ring.near, ring.near_block(k))
        for h in range(2):
            t = 2 * k + h
            to_far(buf_f.at[t], t).wait_recv()
            to_near(buf_f.at[t], t + 2).start()
            if h == 0:
                multiply(buf_n.at[pl.ds(2 * k, 2)], near_owner, 0, mid)
            else:
                multiply(buf_f.at[pl.ds(2 * k, 2)], ring.far_block(k + 1), 0, mid)
            to_near(buf_n.at[t + 2], t + 2).wait_recv()

            @pl.when(t + 2 < n - 2)
            def _():
                to_far(buf_n.at[t + 2], t + 2).start()

            if h == 0:
                multiply(buf_n.at[pl.ds(2 * k, 2)], near_owner, mid, n_parts)
            else:
                multiply(buf_f.at[pl.ds(2 * k, 2)], ring.far_block(k + 1), mid, n_parts)
        return carry

    lax.fori_loop(0, n // 2 - 1, step, 0)
    multiply(buf_n.at[pl.ds(n - 2, 2)], ring.near_block(n // 2 - 1), 0, n_parts)

    def finish(t, carry):
        to_near(own_ref.at[0], t).wait_send()
        return carry

    lax.fori_loop(0, n, finish, 0)

    def finish_far(t, carry):
        to_far(own_ref.at[0], t).wait_send()
        return carry

    lax.fori_loop(0, n - 2, finish_far, 0)


def ring_qkv(normed, w, bias, n):
    _, half, width = normed.shape
    dma = pltpu.SemaphoreType.DMA
    vmem = pl.BlockSpec(memory_space=pltpu.VMEM)
    return pl.pallas_call(
        functools.partial(ring_qkv_kernel, n),
        out_shape=jax.ShapeDtypeStruct((w.shape[0], n, 2, half, 128), BF16),
        in_specs=[vmem, pl.BlockSpec(memory_space=pl.ANY), vmem],
        out_specs=vmem,
        scratch_shapes=[
            pltpu.VMEM(w.shape, BF16),
            pltpu.VMEM((n, half, width), BF16),
            pltpu.VMEM((n - 2, half, width), BF16),
            dma((1,)), dma((n - 2,)), dma((n,)), dma((n - 2,)), dma((n,)),
        ],
        compiler_params=pltpu.CompilerParams(collective_id=2, has_side_effects=True, vmem_limit_bytes=VMEM_LIMIT),
        name="ring_qkv",
    )(normed, w, bias)


def ring_out_kernel(n, slots, qkv_ref, w_ref, embed_ref, bias_ref, out_ref, init_f, add_n, add_f, buf_n, buf_f,
                    send_f, send_n, recv_f, recv_n, free_f, free_n):
    ring = Ring(n)
    heads, head_dim, width = w_ref.shape
    half = embed_ref.shape[1]
    seq_len = qkv_ref.shape[1]
    chunk = width // 4
    scale = head_dim ** -0.5

    def term(block, which, dst):
        first = pl.multiple_of((block * 2 + which) * half, half)
        visible = lax.broadcasted_iota(jnp.int32, (half, seq_len), 1) <= first + lax.broadcasted_iota(jnp.int32, (half, seq_len), 0)
        contexts = []
        for h in range(heads):
            query = qkv_ref[h, pl.ds(first, half), :]
            scores = lax.dot_general(query, qkv_ref[heads + h], (((1,), (1,)), ((), ())), preferred_element_type=F32) * scale
            scores = jnp.where(visible, scores, -jnp.inf)
            scores = jnp.exp(scores - jnp.max(scores, axis=-1, keepdims=True))
            probs = (scores / jnp.sum(scores, axis=-1, keepdims=True)).astype(BF16)
            context = jnp.dot(probs, qkv_ref[2 * heads + h], preferred_element_type=F32).astype(BF16)
            contexts.append(context[:, :head_dim])
        for c in range(width // chunk):
            columns = slice(c * chunk, (c + 1) * chunk)
            total = jnp.dot(contexts[0], w_ref[0, :, columns], preferred_element_type=F32)
            for h in range(1, heads):
                total += jnp.dot(contexts[h], w_ref[h, :, columns], preferred_element_type=F32)
            dst[:, columns] = total

    def near_term(t, dst):
        term(ring.near_block(lax.div(t, 2) + 1), lax.rem(t, 2), dst)

    def far_term(t, dst):
        term(ring.far_block(lax.div(t, 2) + 1), lax.rem(t, 2), dst)

    def to_far(src, t):
        return remote(src, buf_f.at[lax.rem(t, slots)], send_f.at[t], recv_f.at[t], ring.far)

    def to_near(src, t):
        return remote(src, buf_n.at[lax.rem(t, slots)], send_n.at[t], recv_n.at[t], ring.near)

    def pass_far_on(t):
        slot = lax.rem(t, slots)
        to_far(buf_f.at[slot], t).wait_recv()
        buf_f[slot] = buf_f[slot] + add_f[...]

        @pl.when(t + 2 >= slots)
        def _():
            pl.semaphore_wait(free_n, 1)

        to_near(buf_f.at[slot], t + 2).start()

    def pass_near_on(t):
        slot = lax.rem(t, slots)
        to_near(buf_n.at[slot], t).wait_recv()
        buf_n[slot] = buf_n[slot] + add_n[...]

        @pl.when(t >= slots)
        def _():
            pl.semaphore_wait(free_f, 1)

        to_far(buf_n.at[slot], t).start()

    def finish_near(t):
        slot = t % slots
        to_near(buf_n.at[slot], t).wait_recv()
        out_ref[t % 2] = (embed_ref[t % 2].astype(F32) + (buf_n[slot] + add_n[...]) + bias_ref[...]).astype(BF16)

    ring.barrier()

    def begin(t, carry):
        far_term(t, init_f.at[t])
        to_near(init_f.at[t], t).start()
        near_term(t, add_n)
        pass_near_on(t)
        return carry

    lax.fori_loop(0, 2, begin, 0)
    far_term(2, add_f)
    near_term(2, add_n)

    def step(t, carry):
        pass_far_on(t)
        far_term(t + 3, add_f)
        pass_near_on(t + 2)
        near_term(t + 3, add_n)

        @pl.when(t + slots < n - 2)
        def _():
            to_near(init_f.at[0], t + 2).wait_send()
            pl.semaphore_signal(free_f, inc=1, device_id={"tp": ring.far}, device_id_type=MESH)

        @pl.when((t >= 1) & (t - 1 + slots < n))
        def _():
            to_far(init_f.at[0], t - 1).wait_send()
            pl.semaphore_signal(free_n, inc=1, device_id={"tp": ring.near}, device_id_type=MESH)

        return carry

    lax.fori_loop(0, n - 4, step, 0)
    pass_far_on(n - 4)
    far_term(n - 1, add_f)
    finish_near(n - 2)
    near_term(n - 1, add_n)
    pass_far_on(n - 3)
    finish_near(n - 1)

    for t in range(2):
        to_near(init_f.at[0], t).wait_send()

    def finish(t, carry):
        to_near(init_f.at[0], t).wait_send()
        return carry

    lax.fori_loop(n - slots, n, finish, 0)

    def finish_far(t, carry):
        to_far(init_f.at[0], t).wait_send()
        return carry

    lax.fori_loop(n - slots, n - 2, finish_far, 0)


def ring_out(qkv, w_out, embed, b_out, n):
    _, half, width = embed.shape
    slots = n // 2
    dma = pltpu.SemaphoreType.DMA
    vmem = pl.BlockSpec(memory_space=pltpu.VMEM)
    return pl.pallas_call(
        functools.partial(ring_out_kernel, n, slots),
        out_shape=jax.ShapeDtypeStruct((2, half, width), BF16),
        in_specs=[vmem] * 4,
        out_specs=vmem,
        scratch_shapes=[
            pltpu.VMEM((2, half, width), F32),
            pltpu.VMEM((half, width), F32),
            pltpu.VMEM((half, width), F32),
            pltpu.VMEM((slots, half, width), F32),
            pltpu.VMEM((slots, half, width), F32),
            dma((n - 2,)), dma((n,)), dma((n - 2,)), dma((n,)),
            pltpu.SemaphoreType.REGULAR, pltpu.SemaphoreType.REGULAR,
        ],
        compiler_params=pltpu.CompilerParams(collective_id=3, has_side_effects=True, vmem_limit_bytes=VMEM_LIMIT),
        name="ring_out",
    )(qkv, w_out, embed, b_out)


def solution(mesh):
    n = mesh.shape["tp"]

    def local_step(token_ids, word_shard, pos_table, ln_gain, ln_bias, w_qkv, b_qkv, w_out, b_out):
        shard_rows, width = word_shard.shape
        seq_len = token_ids.shape[1]
        block_len = seq_len // n
        half = block_len // 2
        heads, head_dim = w_qkv.shape[2:]
        tp_index = lax.axis_index("tp")

        w = jnp.transpose(w_qkv, (1, 2, 3, 0)).reshape(3 * heads, head_dim, width)
        bias = b_qkv.reshape(3 * heads, 1, head_dim)

        local_ids = token_ids.reshape(seq_len) - tp_index * shard_rows
        partial_rows = gather_rows(local_ids, word_shard, block_len)
        block_rows = ring_sum(partial_rows.reshape(n, 2, half, width), n).reshape(block_len, width)
        pos_block = lax.dynamic_slice_in_dim(pos_table, tp_index * block_len, block_len, axis=0)
        embed = (block_rows.astype(F32) + pos_block.astype(F32)).astype(BF16)
        normed = layer_norm(embed.astype(F32), ln_gain, ln_bias).astype(BF16)
        qkv = ring_qkv(normed.reshape(2, half, width), w, bias, n)
        resid = ring_out(qkv.reshape(3 * heads, seq_len, 128), w_out, embed.reshape(2, half, width), b_out.reshape(1, width), n)
        return resid.reshape(1, block_len, width), embed.reshape(1, block_len, width)

    in_specs = (P("dp", None), P("tp", None), P(None, None), P(None), P(None), P(None, None, "tp", None), P(None, "tp", None), P("tp", None, None), P(None))
    out_specs = (P("dp", "tp", None), P("dp", "tp", None))
    return jax.shard_map(local_step, mesh=mesh, in_specs=in_specs, out_specs=out_specs, check_vma=False)
```

```python
import functools

import jax
import jax.numpy as jnp
from jax import lax
from jax.experimental import pallas as pl
from jax.experimental.pallas import tpu as pltpu
from jax.sharding import PartitionSpec as P

LN_EPS = 1e-5
MESH = pl.DeviceIdType.MESH
BF16 = jnp.bfloat16
F32 = jnp.float32
VMEM_LIMIT = 67043328


def layer_norm(values, gain, bias):
    feat_mean = jnp.mean(values, axis=-1, keepdims=True)
    centered = values - feat_mean
    feat_variance = jnp.mean(centered * centered, axis=-1, keepdims=True)
    return centered * lax.rsqrt(feat_variance + LN_EPS) * gain + bias


ROWS = 16
FETCHES = 16
NONE = -(2**30)


def gather_kernel(block_len, shard_rows, ids_ref, column_ref, table_ref, out_ref, found, count, stamp, fetched, sems):
    j = pl.program_id(0)
    n_blocks = pl.num_programs(0)
    n_groups = shard_rows // ROWS

    def scan(block):
        base = lax.rem(block, 2) * (2 * block_len)

        def one(q, total):
            local_id = ids_ref[block * block_len + q]
            mine = (local_id >= 0) & (local_id < shard_rows)
            group = jnp.where(mine, lax.div(local_id, ROWS), n_groups)
            fresh = mine & (stamp[group] != block)
            stamp[group] = block
            found[base + total] = group
            return total + jnp.where(fresh, 1, 0)

        count[lax.rem(block, 2)] = lax.fori_loop(0, block_len, one, 0, unroll=8)

    def copy_of(block, chunk, k, slot):
        group = found[lax.rem(block, 2) * (2 * block_len) + chunk * FETCHES + k]
        return pltpu.make_async_copy(
            table_ref.at[pl.ds(pl.multiple_of(group * ROWS, ROWS), ROWS), :],
            fetched.at[slot, pl.ds(pl.multiple_of(k * ROWS, ROWS), ROWS), :],
            sems.at[slot, k],
        )

    def in_chunk(block, chunk):
        return jnp.minimum(count[lax.rem(block, 2)] - chunk * FETCHES, FETCHES)

    def start(block, chunk, slot):
        def one(k, carry):
            copy_of(block, chunk, k, slot).start()
            return carry

        lax.fori_loop(0, in_chunk(block, chunk), one, 0)

    def wait(block, chunk, slot):
        def one(k, carry):
            copy_of(block, chunk, k, slot).wait()
            return carry

        lax.fori_loop(0, in_chunk(block, chunk), one, 0)

    def selector(block, chunk):
        columns = lax.broadcasted_iota(jnp.int32, (1, FETCHES * ROWS), 1)
        base = lax.rem(block, 2) * (2 * block_len) + chunk * FETCHES
        held = in_chunk(block, chunk)
        first = jnp.full((1, FETCHES * ROWS), NONE, jnp.int32)
        for k in range(FETCHES):
            first = jnp.where(lax.div(columns, ROWS) == k, jnp.where(k < held, found[base + k] * ROWS, NONE), first)
        return jnp.where(column_ref[...] == first + lax.rem(columns, ROWS), 1.0, 0.0).astype(BF16)

    @pl.when(j == 0)
    def _():
        fetched[...] = jnp.zeros_like(fetched)

        def clear(g, carry):
            stamp[g] = -1
            return carry

        lax.fori_loop(0, n_groups + 1, clear, 0)
        scan(0)
        start(0, 0, 0)

    @pl.when(j + 1 < n_blocks)
    def _():
        scan(j + 1)
        start(j + 1, 0, lax.rem(j + 1, 2))

    slot = lax.rem(j, 2)
    wait(j, 0, slot)
    out_ref[...] = jnp.dot(selector(j, 0), fetched[slot], preferred_element_type=F32).astype(BF16)

    def more(chunk, carry):
        start(j, chunk, slot)
        wait(j, chunk, slot)
        out_ref[...] += jnp.dot(selector(j, chunk), fetched[slot], preferred_element_type=F32).astype(BF16)
        return carry

    lax.fori_loop(1, lax.div(count[slot] + (FETCHES - 1), FETCHES), more, 0)


def gather_rows(local_ids, table, block_len):
    (n_ids,), (shard_rows, width) = local_ids.shape, table.shape
    return pl.pallas_call(
        functools.partial(gather_kernel, block_len, shard_rows),
        grid=(n_ids // block_len,),
        out_shape=jax.ShapeDtypeStruct((n_ids, width), BF16),
        in_specs=[
            pl.BlockSpec(memory_space=pltpu.SMEM),
            pl.BlockSpec((block_len, 1), lambda j: (j, 0)),
            pl.BlockSpec(memory_space=pl.ANY),
        ],
        out_specs=pl.BlockSpec((block_len, width), lambda j: (j, 0)),
        scratch_shapes=[
            pltpu.SMEM((4 * block_len,), jnp.int32),
            pltpu.SMEM((2,), jnp.int32),
            pltpu.SMEM((shard_rows // ROWS + 1,), jnp.int32),
            pltpu.VMEM((2, FETCHES * ROWS, width), BF16),
            pltpu.SemaphoreType.DMA((2, FETCHES)),
        ],
        compiler_params=pltpu.CompilerParams(vmem_limit_bytes=40 * 2**20),
        name="gather_rows",
    )(local_ids, local_ids.reshape(n_ids, 1), table)


class Ring:
    def __init__(self, n):
        self.chips = n // 2
        self.me = lax.axis_index("tp")
        self.odd = lax.rem(self.me, 2)
        self.chip = lax.div(self.me, 2)
        self.way = 2 * self.odd - 1
        self.near = self.me - self.way
        self.far = lax.rem(self.me + self.way + n, n)

    def near_block(self, k):
        return 2 * lax.rem(self.chip - self.way * k + 2 * self.chips, self.chips) + self.odd

    def far_block(self, k):
        return 2 * lax.rem(self.chip + self.way * k + 2 * self.chips, self.chips) + 1 - self.odd

    def barrier(self):
        sem = pltpu.get_barrier_semaphore()
        for device in (self.near, self.far):
            pl.semaphore_signal(sem, inc=1, device_id={"tp": device}, device_id_type=MESH)
        pl.semaphore_wait(sem, 2)


def remote(src, dst, send_sem, recv_sem, device):
    return pltpu.make_async_remote_copy(
        src_ref=src, dst_ref=dst, send_sem=send_sem, recv_sem=recv_sem, device_id={"tp": device}, device_id_type=MESH
    )


def ring_sum_kernel(n, part_ref, out_ref, own_n, own_f, buf_n, buf_f, own_sem, send_f, send_n, recv_f, recv_n):
    ring = Ring(n)

    def load_n(t):
        return pltpu.make_async_copy(part_ref.at[ring.near_block(lax.div(t, 2) + 1), lax.rem(t, 2)], own_n.at[t], own_sem.at[0, t])

    def load_f(t):
        return pltpu.make_async_copy(part_ref.at[ring.far_block(lax.div(t, 2) + 1), lax.rem(t, 2)], own_f.at[t], own_sem.at[1, t])

    def start_loads(t, carry):
        load_f(t).start()
        load_n(t).start()
        return carry

    lax.fori_loop(0, n, start_loads, 0)
    ring.barrier()

    def to_far(src, t):
        return remote(src, buf_f.at[t], send_f.at[t], recv_f.at[t], ring.far)

    def to_near(src, t):
        return remote(src, buf_n.at[t], send_n.at[t], recv_n.at[t], ring.near)

    def pass_far_on(t):
        to_far(buf_f.at[t], t).wait_recv()
        load_f(t + 2).wait()
        buf_f[t] = buf_f[t] + own_f[t + 2]
        to_near(buf_f.at[t], t + 2).start()

    def take_near(t):
        to_near(buf_n.at[t], t).wait_recv()
        load_n(t).wait()

    def pass_near_on(t):
        take_near(t)
        buf_n[t] = buf_n[t] + own_n[t]
        to_far(buf_n.at[t], t).start()

    def finish_near(t):
        take_near(t)
        out_ref[t % 2] = buf_n[t] + own_n[t]

    for t in range(2):
        load_f(t).wait()
        to_near(own_f.at[t], t).start()
    for t in range(2):
        pass_near_on(t)

    def step(t, carry):
        pass_far_on(t)
        pass_near_on(t + 2)
        return carry

    lax.fori_loop(0, n - 4, step, 0)
    for t in (n - 4, n - 3):
        pass_far_on(t)
        finish_near(t + 2)

    def finish(t, carry):
        to_near(own_f.at[t], t).wait_send()
        return carry

    lax.fori_loop(0, n, finish, 0)

    def finish_far(t, carry):
        to_far(buf_n.at[t], t).wait_send()
        return carry

    lax.fori_loop(0, n - 2, finish_far, 0)


def ring_sum(partial_rows, n):
    _, _, half, width = partial_rows.shape
    dma = pltpu.SemaphoreType.DMA
    return pl.pallas_call(
        functools.partial(ring_sum_kernel, n),
        out_shape=jax.ShapeDtypeStruct((2, half, width), BF16),
        in_specs=[pl.BlockSpec(memory_space=pl.ANY)],
        out_specs=pl.BlockSpec(memory_space=pltpu.VMEM),
        scratch_shapes=[
            pltpu.VMEM((n, half, width), BF16),
            pltpu.VMEM((n, half, width), BF16),
            pltpu.VMEM((n, half, width), BF16),
            pltpu.VMEM((n - 2, half, width), BF16),
            dma((2, n)), dma((n - 2,)), dma((n,)), dma((n - 2,)), dma((n,)),
        ],
        compiler_params=pltpu.CompilerParams(collective_id=1, has_side_effects=True, vmem_limit_bytes=VMEM_LIMIT),
        name="ring_sum",
    )(partial_rows)


def ring_qkv_kernel(n, own_hbm, w_hbm, bias_ref, out_ref, w_ref, buf, load_sem, send_f, send_n, recv_f, recv_n):
    ring = Ring(n)
    _, _, half, width = buf.shape
    n_parts, part_width = w_ref.shape[:2]
    load_own = pltpu.make_async_copy(own_hbm, buf.at[0, pl.ds(2, 2)], load_sem.at[0])
    load_own.start()
    load_w = pltpu.make_async_copy(w_hbm, w_ref, load_sem.at[1])
    load_w.start()
    ring.barrier()

    def near_slot(t):
        return buf.at[lax.div(t, 2), lax.rem(t, 2)]

    def far_slot(t):
        return buf.at[lax.div(t, 2) + 1, 2 + lax.rem(t, 2)]

    def to_far(src, t):
        return remote(src, far_slot(t), send_f.at[t], recv_f.at[t], ring.far)

    def to_near(src, t):
        return remote(src, near_slot(t), send_n.at[t], recv_n.at[t], ring.near)

    def multiply(k, low, high):
        near_owner = jnp.where(k == 0, ring.near, ring.near_block(k))
        far_owner = jnp.where(k == 0, ring.me, ring.far_block(k))

        def one(c, carry):
            product = lax.dot_general(
                buf[k].reshape(4 * half, width), w_ref[c], (((1,), (1,)), ((), ())), preferred_element_type=F32
            )
            product = (product + bias_ref[c]).astype(BF16).reshape(2, 2, half, part_width)
            out_ref[c, near_owner, :, :, :part_width] = product[0]
            out_ref[c, far_owner, :, :, :part_width] = product[1]
            return carry

        lax.fori_loop(low, high, one, 0)

    load_own.wait()
    for t in range(2):
        to_far(buf.at[0, 2 + t], t).start()
    for t in range(2):
        to_near(buf.at[0, 2 + t], t).start()
    out_ref[...] = jnp.zeros_like(out_ref)
    for t in range(2):
        to_near(near_slot(t), t).wait_recv()
    load_w.wait()
    quarter = n_parts // 4

    def step(k, carry):
        for h in range(2):
            t = 2 * k + h
            to_far(far_slot(t), t).wait_recv()
            to_near(far_slot(t), t + 2).start()
            multiply(k, 2 * h * quarter, (2 * h + 1) * quarter)
            to_near(near_slot(t + 2), t + 2).wait_recv()

            @pl.when(t + 2 < n - 2)
            def _():
                to_far(near_slot(t + 2), t + 2).start()

            multiply(k, (2 * h + 1) * quarter, n_parts if h else 2 * quarter)
        return carry

    lax.fori_loop(0, n // 2 - 1, step, 0)
    multiply(n // 2 - 1, 0, n_parts)

    def finish(t, carry):
        to_near(buf.at[0, 0], t).wait_send()
        return carry

    lax.fori_loop(0, n, finish, 0)

    def finish_far(t, carry):
        to_far(buf.at[0, 0], t).wait_send()
        return carry

    lax.fori_loop(0, n - 2, finish_far, 0)


def ring_qkv(normed, w, bias, n):
    _, half, width = normed.shape
    dma = pltpu.SemaphoreType.DMA
    vmem = pl.BlockSpec(memory_space=pltpu.VMEM)
    return pl.pallas_call(
        functools.partial(ring_qkv_kernel, n),
        out_shape=jax.ShapeDtypeStruct((w.shape[0], n, 2, half, 128), BF16),
        in_specs=[pl.BlockSpec(memory_space=pl.ANY), pl.BlockSpec(memory_space=pl.ANY), vmem],
        out_specs=vmem,
        scratch_shapes=[
            pltpu.VMEM(w.shape, BF16),
            pltpu.VMEM((n // 2, 4, half, width), BF16),
            dma((2,)), dma((n - 2,)), dma((n,)), dma((n - 2,)), dma((n,)),
        ],
        compiler_params=pltpu.CompilerParams(collective_id=2, has_side_effects=True, vmem_limit_bytes=VMEM_LIMIT),
        name="ring_qkv",
    )(normed, w, bias)


def ring_out_kernel(n, slots, qkv_ref, w_ref, embed_ref, bias_ref, out_ref, init_f, add_n, add_f, buf_n, buf_f,
                    send_f, send_n, recv_f, recv_n, free_f, free_n):
    ring = Ring(n)
    heads, head_dim, width = w_ref.shape
    half = embed_ref.shape[1]
    seq_len = qkv_ref.shape[1]
    chunk = width // 4
    scale = head_dim ** -0.5

    def term(block, which, dst):
        first = pl.multiple_of((block * 2 + which) * half, half)
        visible = lax.broadcasted_iota(jnp.int32, (half, seq_len), 1) <= first + lax.broadcasted_iota(jnp.int32, (half, seq_len), 0)
        contexts = []
        for h in range(heads):
            query = qkv_ref[h, pl.ds(first, half), :]
            scores = lax.dot_general(query, qkv_ref[heads + h], (((1,), (1,)), ((), ())), preferred_element_type=F32) * scale
            scores = jnp.where(visible, scores, -jnp.inf)
            scores = jnp.exp(scores - jnp.max(scores, axis=-1, keepdims=True))
            probs = (scores / jnp.sum(scores, axis=-1, keepdims=True)).astype(BF16)
            context = jnp.dot(probs, qkv_ref[2 * heads + h], preferred_element_type=F32).astype(BF16)
            contexts.append(context[:, :head_dim])
        for c in range(width // chunk):
            columns = slice(c * chunk, (c + 1) * chunk)
            total = jnp.dot(contexts[0], w_ref[0, :, columns], preferred_element_type=F32)
            for h in range(1, heads):
                total += jnp.dot(contexts[h], w_ref[h, :, columns], preferred_element_type=F32)
            dst[:, columns] = total

    def near_term(t, dst):
        term(ring.near_block(lax.div(t, 2) + 1), lax.rem(t, 2), dst)

    def far_term(t, dst):
        term(ring.far_block(lax.div(t, 2) + 1), lax.rem(t, 2), dst)

    def to_far(src, t):
        return remote(src, buf_f.at[lax.rem(t, slots)], send_f.at[t], recv_f.at[t], ring.far)

    def to_near(src, t):
        return remote(src, buf_n.at[lax.rem(t, slots)], send_n.at[t], recv_n.at[t], ring.near)

    def pass_far_on(t):
        slot = lax.rem(t, slots)
        to_far(buf_f.at[slot], t).wait_recv()
        buf_f[slot] = buf_f[slot] + add_f[...]

        @pl.when(t + 2 >= slots)
        def _():
            pl.semaphore_wait(free_n, 1)

        to_near(buf_f.at[slot], t + 2).start()

    def pass_near_on(t):
        slot = lax.rem(t, slots)
        to_near(buf_n.at[slot], t).wait_recv()
        buf_n[slot] = buf_n[slot] + add_n[...]

        @pl.when(t >= slots)
        def _():
            pl.semaphore_wait(free_f, 1)

        to_far(buf_n.at[slot], t).start()

    def finish_near(t):
        slot = t % slots
        to_near(buf_n.at[slot], t).wait_recv()
        out_ref[t % 2] = (embed_ref[t % 2].astype(F32) + (buf_n[slot] + add_n[...]) + bias_ref[...]).astype(BF16)

    ring.barrier()

    def begin(t, carry):
        far_term(t, init_f.at[t])
        to_near(init_f.at[t], t).start()
        near_term(t, add_n)
        pass_near_on(t)
        return carry

    lax.fori_loop(0, 2, begin, 0)
    far_term(2, add_f)
    near_term(2, add_n)

    def step(t, carry):
        pass_far_on(t)
        far_term(t + 3, add_f)
        pass_near_on(t + 2)
        near_term(t + 3, add_n)

        @pl.when(t + slots < n - 2)
        def _():
            to_near(init_f.at[0], t + 2).wait_send()
            pl.semaphore_signal(free_f, inc=1, device_id={"tp": ring.far}, device_id_type=MESH)

        @pl.when((t >= 1) & (t - 1 + slots < n))
        def _():
            to_far(init_f.at[0], t - 1).wait_send()
            pl.semaphore_signal(free_n, inc=1, device_id={"tp": ring.near}, device_id_type=MESH)

        return carry

    lax.fori_loop(0, n - 4, step, 0)
    pass_far_on(n - 4)
    far_term(n - 1, add_f)
    finish_near(n - 2)
    near_term(n - 1, add_n)
    pass_far_on(n - 3)
    finish_near(n - 1)

    for t in range(2):
        to_near(init_f.at[0], t).wait_send()

    def finish(t, carry):
        to_near(init_f.at[0], t).wait_send()
        return carry

    lax.fori_loop(n - slots, n, finish, 0)

    def finish_far(t, carry):
        to_far(init_f.at[0], t).wait_send()
        return carry

    lax.fori_loop(n - slots, n - 2, finish_far, 0)


def ring_out(qkv, w_out, embed, b_out, n):
    _, half, width = embed.shape
    slots = n // 2
    dma = pltpu.SemaphoreType.DMA
    vmem = pl.BlockSpec(memory_space=pltpu.VMEM)
    return pl.pallas_call(
        functools.partial(ring_out_kernel, n, slots),
        out_shape=jax.ShapeDtypeStruct((2, half, width), BF16),
        in_specs=[vmem] * 4,
        out_specs=vmem,
        scratch_shapes=[
            pltpu.VMEM((2, half, width), F32),
            pltpu.VMEM((half, width), F32),
            pltpu.VMEM((half, width), F32),
            pltpu.VMEM((slots, half, width), F32),
            pltpu.VMEM((slots, half, width), F32),
            dma((n - 2,)), dma((n,)), dma((n - 2,)), dma((n,)),
            pltpu.SemaphoreType.REGULAR, pltpu.SemaphoreType.REGULAR,
        ],
        compiler_params=pltpu.CompilerParams(collective_id=3, has_side_effects=True, vmem_limit_bytes=VMEM_LIMIT),
        name="ring_out",
    )(qkv, w_out, embed, b_out)


LIMIT = 16


def pick_kernel(want_ref, column_ref, table_ref, out_ref, fetched, sems):
    j = pl.program_id(0)

    def each(block, slot, act):
        def one(k, carry):
            row = want_ref[block * LIMIT + k]

            @pl.when(row >= 0)
            def _():
                start = pl.multiple_of(lax.div(row, ROWS) * ROWS, ROWS)
                act(pltpu.make_async_copy(
                    table_ref.at[pl.ds(start, ROWS), :],
                    fetched.at[slot, pl.ds(pl.multiple_of(k * ROWS, ROWS), ROWS), :],
                    sems.at[slot, k],
                ))

            return carry

        lax.fori_loop(0, LIMIT, one, 0)

    @pl.when(j == 0)
    def _():
        fetched[...] = jnp.zeros_like(fetched)
        each(0, 0, lambda copy: copy.start())

    @pl.when(j + 1 < pl.num_programs(0))
    def _():
        each(j + 1, lax.rem(j + 1, 2), lambda copy: copy.start())

    slot = lax.rem(j, 2)
    columns = lax.broadcasted_iota(jnp.int32, (LIMIT, LIMIT * ROWS), 1)
    place = lax.broadcasted_iota(jnp.int32, (LIMIT, LIMIT * ROWS), 0) * ROWS
    row = column_ref[...]
    selector = jnp.where((row >= 0) & (columns == place + lax.rem(jnp.maximum(row, 0), ROWS)), 1.0, 0.0).astype(BF16)
    each(j, slot, lambda copy: copy.wait())
    out_ref[...] = jnp.dot(selector, fetched[slot], preferred_element_type=F32).astype(BF16)


def pick_rows(want, table, n):
    width = table.shape[1]
    return pl.pallas_call(
        pick_kernel,
        grid=(n,),
        out_shape=jax.ShapeDtypeStruct((n * LIMIT, width), BF16),
        in_specs=[
            pl.BlockSpec(memory_space=pltpu.SMEM),
            pl.BlockSpec((LIMIT, 1), lambda j: (j, 0)),
            pl.BlockSpec(memory_space=pl.ANY),
        ],
        out_specs=pl.BlockSpec((LIMIT, width), lambda j: (j, 0)),
        scratch_shapes=[pltpu.VMEM((2, LIMIT * ROWS, width), BF16), pltpu.SemaphoreType.DMA((2, LIMIT))],
        compiler_params=pltpu.CompilerParams(vmem_limit_bytes=VMEM_LIMIT),
        name="pick_rows",
    )(want, want.reshape(n * LIMIT, 1), table)


def exchange_kernel(n, picked_ref, index_ref, out_ref, got, own_sem, send, recv):
    me = lax.axis_index("tp")
    own = pltpu.make_async_copy(picked_ref.at[me], got.at[me], own_sem.at[0])
    own.start()
    barrier = pltpu.get_barrier_semaphore()

    def greet(j, carry):
        pl.semaphore_signal(barrier, inc=1, device_id={"tp": lax.rem(me + j, n)}, device_id_type=MESH)
        return carry

    lax.fori_loop(1, n, greet, 0)
    pl.semaphore_wait(barrier, n - 1)

    def copy_to(j):
        other = lax.rem(me + j, n)
        return remote(picked_ref.at[other], got.at[me], send.at[j], recv.at[j], other)

    for j in range(n // 2, 0, -1):
        copy_to(j).start()
        if j < n // 2:
            copy_to(n - j).start()

    def arrive(j, carry):
        source = lax.rem(me - j + n, n)
        remote(picked_ref.at[0], got.at[source], send.at[j], recv.at[j], source).wait_recv()
        return carry

    lax.fori_loop(1, n, arrive, 0)
    own.wait()
    block_len, width = out_ref.shape
    rows = n * LIMIT
    selector = jnp.where(lax.broadcasted_iota(jnp.int32, (block_len, rows), 1) == index_ref[...], 1.0, 0.0).astype(BF16)
    chunk = width // 4
    for c in range(4):
        columns = slice(c * chunk, (c + 1) * chunk)
        out_ref[:, columns] = jnp.dot(
            selector, got[:, :, columns].reshape(rows, chunk), preferred_element_type=F32
        ).astype(BF16)

    def sent(j, carry):
        copy_to(j).wait_send()
        return carry

    lax.fori_loop(1, n, sent, 0)


def exchange(picked, index, n):
    _, _, width = picked.shape
    dma = pltpu.SemaphoreType.DMA
    vmem = pl.BlockSpec(memory_space=pltpu.VMEM)
    return pl.pallas_call(
        functools.partial(exchange_kernel, n),
        out_shape=jax.ShapeDtypeStruct((index.shape[0], width), BF16),
        in_specs=[pl.BlockSpec(memory_space=pl.ANY), vmem],
        out_specs=vmem,
        scratch_shapes=[pltpu.VMEM((n, LIMIT, width), BF16), dma((1,)), dma((n,)), dma((n,))],
        compiler_params=pltpu.CompilerParams(collective_id=4, has_side_effects=True, vmem_limit_bytes=VMEM_LIMIT),
        name="exchange",
    )(picked, index)


def look_up(token_ids, table, n):
    shard_rows, width = table.shape
    me = lax.axis_index("tp")
    ids = token_ids.reshape(n, -1)
    block_len = ids.shape[1]
    earlier = lax.broadcasted_iota(jnp.int32, (block_len, block_len), 0) > lax.broadcasted_iota(jnp.int32, (block_len, block_len), 1)
    same = ids[:, :, None] == ids[:, None, :]
    fresh = jnp.sum((same & earlier[None]).astype(jnp.int32), axis=2) == 0
    owner = lax.div(ids, shard_rows)
    rank = jnp.sum(((owner[:, :, None] == owner[:, None, :]) & earlier[None] & fresh[:, None, :]).astype(jnp.int32), axis=2)
    overflow = jnp.max(jnp.where(fresh, rank, 0)) >= LIMIT
    places = lax.broadcasted_iota(jnp.int32, (n, LIMIT, block_len), 1)
    wanted = (places == rank[:, None, :]) & (fresh & (owner == me))[:, None, :]
    want = jnp.sum(jnp.where(wanted, (ids - me * shard_rows)[:, None, :] + 1, 0), axis=2) - 1

    my_ids = lax.dynamic_index_in_dim(ids, me, 0, keepdims=False)
    my_slots = lax.dynamic_index_in_dim(jnp.where(fresh, owner * LIMIT + rank, 0), me, 0, keepdims=False)
    my_fresh = lax.dynamic_index_in_dim(fresh, me, 0, keepdims=False)
    match = (my_ids[:, None] == my_ids[None, :]) & my_fresh[None, :]
    index = jnp.sum(jnp.where(match, my_slots[None, :], 0), axis=1)

    def by_exchange():
        return exchange(pick_rows(want.reshape(n * LIMIT), table, n).reshape(n, LIMIT, width), index.reshape(block_len, 1), n)

    def by_sum():
        local_ids = token_ids.reshape(n * block_len) - me * shard_rows
        partial_rows = gather_rows(local_ids, table, block_len)
        return ring_sum(partial_rows.reshape(n, 2, block_len // 2, width), n).reshape(block_len, width)

    return lax.cond(overflow, by_sum, by_exchange)


def solution(mesh):
    n = mesh.shape["tp"]

    def local_step(token_ids, word_shard, pos_table, ln_gain, ln_bias, w_qkv, b_qkv, w_out, b_out):
        width = word_shard.shape[1]
        seq_len = token_ids.shape[1]
        block_len = seq_len // n
        half = block_len // 2
        heads, head_dim = w_qkv.shape[2:]
        tp_index = lax.axis_index("tp")

        w = jnp.transpose(w_qkv, (1, 2, 3, 0)).reshape(3 * heads, head_dim, width)
        bias = b_qkv.reshape(3 * heads, 1, head_dim)

        block_rows = look_up(token_ids.reshape(seq_len), word_shard, n)
        pos_block = lax.dynamic_slice_in_dim(pos_table, tp_index * block_len, block_len, axis=0)
        embed = (block_rows.astype(F32) + pos_block.astype(F32)).astype(BF16)
        normed = layer_norm(embed.astype(F32), ln_gain, ln_bias).astype(BF16)
        qkv = ring_qkv(normed.reshape(2, half, width), w, bias, n)
        resid = ring_out(qkv.reshape(3 * heads, seq_len, 128), w_out, embed.reshape(2, half, width), b_out.reshape(1, width), n)
        return resid.reshape(1, block_len, width), embed.reshape(1, block_len, width)

    in_specs = (P("dp", None), P("tp", None), P(None, None), P(None), P(None), P(None, None, "tp", None), P(None, "tp", None), P("tp", None, None), P(None))
    out_specs = (P("dp", "tp", None), P("dp", "tp", None))
    return jax.shard_map(local_step, mesh=mesh, in_specs=in_specs, out_specs=out_specs, check_vma=False)
```

```python
import functools

import jax
import jax.numpy as jnp
from jax import lax
from jax.experimental import pallas as pl
from jax.experimental.pallas import tpu as pltpu
from jax.sharding import PartitionSpec as P

LN_EPS = 1e-5
MESH = pl.DeviceIdType.MESH
BF16 = jnp.bfloat16
F32 = jnp.float32
VMEM_LIMIT = 67043328


def layer_norm(values, gain, bias):
    feat_mean = jnp.mean(values, axis=-1, keepdims=True)
    centered = values - feat_mean
    feat_variance = jnp.mean(centered * centered, axis=-1, keepdims=True)
    return centered * lax.rsqrt(feat_variance + LN_EPS) * gain + bias


ROWS = 16
FETCHES = 16
NONE = -(2**30)


def gather_kernel(block_len, shard_rows, ids_ref, column_ref, table_ref, out_ref, found, count, stamp, fetched, sems):
    j = pl.program_id(0)
    n_blocks = pl.num_programs(0)
    n_groups = shard_rows // ROWS

    def scan(block):
        base = lax.rem(block, 2) * (2 * block_len)

        def one(q, total):
            local_id = ids_ref[block * block_len + q]
            mine = (local_id >= 0) & (local_id < shard_rows)
            group = jnp.where(mine, lax.div(local_id, ROWS), n_groups)
            fresh = mine & (stamp[group] != block)
            stamp[group] = block
            found[base + total] = group
            return total + jnp.where(fresh, 1, 0)

        count[lax.rem(block, 2)] = lax.fori_loop(0, block_len, one, 0, unroll=8)

    def copy_of(block, chunk, k, slot):
        group = found[lax.rem(block, 2) * (2 * block_len) + chunk * FETCHES + k]
        return pltpu.make_async_copy(
            table_ref.at[pl.ds(pl.multiple_of(group * ROWS, ROWS), ROWS), :],
            fetched.at[slot, pl.ds(pl.multiple_of(k * ROWS, ROWS), ROWS), :],
            sems.at[slot, k],
        )

    def in_chunk(block, chunk):
        return jnp.minimum(count[lax.rem(block, 2)] - chunk * FETCHES, FETCHES)

    def start(block, chunk, slot):
        def one(k, carry):
            copy_of(block, chunk, k, slot).start()
            return carry

        lax.fori_loop(0, in_chunk(block, chunk), one, 0)

    def wait(block, chunk, slot):
        def one(k, carry):
            copy_of(block, chunk, k, slot).wait()
            return carry

        lax.fori_loop(0, in_chunk(block, chunk), one, 0)

    def selector(block, chunk):
        columns = lax.broadcasted_iota(jnp.int32, (1, FETCHES * ROWS), 1)
        base = lax.rem(block, 2) * (2 * block_len) + chunk * FETCHES
        held = in_chunk(block, chunk)
        first = jnp.full((1, FETCHES * ROWS), NONE, jnp.int32)
        for k in range(FETCHES):
            first = jnp.where(lax.div(columns, ROWS) == k, jnp.where(k < held, found[base + k] * ROWS, NONE), first)
        return jnp.where(column_ref[...] == first + lax.rem(columns, ROWS), 1.0, 0.0).astype(BF16)

    @pl.when(j == 0)
    def _():
        fetched[...] = jnp.zeros_like(fetched)

        def clear(g, carry):
            stamp[g] = -1
            return carry

        lax.fori_loop(0, n_groups + 1, clear, 0)
        scan(0)
        start(0, 0, 0)

    @pl.when(j + 1 < n_blocks)
    def _():
        scan(j + 1)
        start(j + 1, 0, lax.rem(j + 1, 2))

    slot = lax.rem(j, 2)
    wait(j, 0, slot)
    out_ref[...] = jnp.dot(selector(j, 0), fetched[slot], preferred_element_type=F32).astype(BF16)

    def more(chunk, carry):
        start(j, chunk, slot)
        wait(j, chunk, slot)
        out_ref[...] += jnp.dot(selector(j, chunk), fetched[slot], preferred_element_type=F32).astype(BF16)
        return carry

    lax.fori_loop(1, lax.div(count[slot] + (FETCHES - 1), FETCHES), more, 0)


def gather_rows(local_ids, table, block_len):
    (n_ids,), (shard_rows, width) = local_ids.shape, table.shape
    return pl.pallas_call(
        functools.partial(gather_kernel, block_len, shard_rows),
        grid=(n_ids // block_len,),
        out_shape=jax.ShapeDtypeStruct((n_ids, width), BF16),
        in_specs=[
            pl.BlockSpec(memory_space=pltpu.SMEM),
            pl.BlockSpec((block_len, 1), lambda j: (j, 0)),
            pl.BlockSpec(memory_space=pl.ANY),
        ],
        out_specs=pl.BlockSpec((block_len, width), lambda j: (j, 0)),
        scratch_shapes=[
            pltpu.SMEM((4 * block_len,), jnp.int32),
            pltpu.SMEM((2,), jnp.int32),
            pltpu.SMEM((shard_rows // ROWS + 1,), jnp.int32),
            pltpu.VMEM((2, FETCHES * ROWS, width), BF16),
            pltpu.SemaphoreType.DMA((2, FETCHES)),
        ],
        compiler_params=pltpu.CompilerParams(vmem_limit_bytes=40 * 2**20),
        name="gather_rows",
    )(local_ids, local_ids.reshape(n_ids, 1), table)


class Ring:
    def __init__(self, n):
        self.chips = n // 2
        self.me = lax.axis_index("tp")
        self.odd = lax.rem(self.me, 2)
        self.chip = lax.div(self.me, 2)
        self.way = 2 * self.odd - 1
        self.near = self.me - self.way
        self.far = lax.rem(self.me + self.way + n, n)

    def near_block(self, k):
        return 2 * lax.rem(self.chip - self.way * k + 2 * self.chips, self.chips) + self.odd

    def far_block(self, k):
        return 2 * lax.rem(self.chip + self.way * k + 2 * self.chips, self.chips) + 1 - self.odd

    def barrier(self):
        sem = pltpu.get_barrier_semaphore()
        for device in (self.near, self.far):
            pl.semaphore_signal(sem, inc=1, device_id={"tp": device}, device_id_type=MESH)
        pl.semaphore_wait(sem, 2)


def remote(src, dst, send_sem, recv_sem, device):
    return pltpu.make_async_remote_copy(
        src_ref=src, dst_ref=dst, send_sem=send_sem, recv_sem=recv_sem, device_id={"tp": device}, device_id_type=MESH
    )


def ring_sum_kernel(n, part_ref, out_ref, own_n, own_f, buf_n, buf_f, own_sem, send_f, send_n, recv_f, recv_n):
    ring = Ring(n)

    def load_n(t):
        return pltpu.make_async_copy(part_ref.at[ring.near_block(lax.div(t, 2) + 1), lax.rem(t, 2)], own_n.at[t], own_sem.at[0, t])

    def load_f(t):
        return pltpu.make_async_copy(part_ref.at[ring.far_block(lax.div(t, 2) + 1), lax.rem(t, 2)], own_f.at[t], own_sem.at[1, t])

    def start_loads(t, carry):
        load_f(t).start()
        load_n(t).start()
        return carry

    lax.fori_loop(0, n, start_loads, 0)
    ring.barrier()

    def to_far(src, t):
        return remote(src, buf_f.at[t], send_f.at[t], recv_f.at[t], ring.far)

    def to_near(src, t):
        return remote(src, buf_n.at[t], send_n.at[t], recv_n.at[t], ring.near)

    def pass_far_on(t):
        to_far(buf_f.at[t], t).wait_recv()
        load_f(t + 2).wait()
        buf_f[t] = buf_f[t] + own_f[t + 2]
        to_near(buf_f.at[t], t + 2).start()

    def take_near(t):
        to_near(buf_n.at[t], t).wait_recv()
        load_n(t).wait()

    def pass_near_on(t):
        take_near(t)
        buf_n[t] = buf_n[t] + own_n[t]
        to_far(buf_n.at[t], t).start()

    def finish_near(t):
        take_near(t)
        out_ref[t % 2] = buf_n[t] + own_n[t]

    for t in range(2):
        load_f(t).wait()
        to_near(own_f.at[t], t).start()
    for t in range(2):
        pass_near_on(t)

    def step(t, carry):
        pass_far_on(t)
        pass_near_on(t + 2)
        return carry

    lax.fori_loop(0, n - 4, step, 0)
    for t in (n - 4, n - 3):
        pass_far_on(t)
        finish_near(t + 2)

    def finish(t, carry):
        to_near(own_f.at[t], t).wait_send()
        return carry

    lax.fori_loop(0, n, finish, 0)

    def finish_far(t, carry):
        to_far(buf_n.at[t], t).wait_send()
        return carry

    lax.fori_loop(0, n - 2, finish_far, 0)


def ring_sum(partial_rows, n):
    _, _, half, width = partial_rows.shape
    dma = pltpu.SemaphoreType.DMA
    return pl.pallas_call(
        functools.partial(ring_sum_kernel, n),
        out_shape=jax.ShapeDtypeStruct((2, half, width), BF16),
        in_specs=[pl.BlockSpec(memory_space=pl.ANY)],
        out_specs=pl.BlockSpec(memory_space=pltpu.VMEM),
        scratch_shapes=[
            pltpu.VMEM((n, half, width), BF16),
            pltpu.VMEM((n, half, width), BF16),
            pltpu.VMEM((n, half, width), BF16),
            pltpu.VMEM((n - 2, half, width), BF16),
            dma((2, n)), dma((n - 2,)), dma((n,)), dma((n - 2,)), dma((n,)),
        ],
        compiler_params=pltpu.CompilerParams(collective_id=1, has_side_effects=True, vmem_limit_bytes=VMEM_LIMIT),
        name="ring_sum",
    )(partial_rows)


def ring_qkv_kernel(n, pack, own_hbm, w_hbm, bias_ref, out_ref, w_ref, buf, load_sem, send_f, send_n, recv_f, recv_n):
    ring = Ring(n)
    _, _, half, width = buf.shape
    n_parts, part_width = w_ref.shape[:2]
    head_dim = part_width // pack
    load_own = pltpu.make_async_copy(own_hbm, buf.at[0, pl.ds(2, 2)], load_sem.at[0])
    load_own.start()
    load_w = pltpu.make_async_copy(w_hbm, w_ref, load_sem.at[1])
    load_w.start()
    ring.barrier()

    def near_slot(t):
        return buf.at[lax.div(t, 2), lax.rem(t, 2)]

    def far_slot(t):
        return buf.at[lax.div(t, 2) + 1, 2 + lax.rem(t, 2)]

    def to_far(src, t):
        return remote(src, far_slot(t), send_f.at[t], recv_f.at[t], ring.far)

    def to_near(src, t):
        return remote(src, near_slot(t), send_n.at[t], recv_n.at[t], ring.near)

    def multiply(k, low, high):
        near_owner = jnp.where(k == 0, ring.near, ring.near_block(k))
        far_owner = jnp.where(k == 0, ring.me, ring.far_block(k))

        def one(c, carry):
            product = lax.dot_general(
                buf[k].reshape(4 * half, width), w_ref[c], (((1,), (1,)), ((), ())), preferred_element_type=F32
            )
            product = (product + bias_ref[c]).astype(BF16)
            for i in range(pack):
                piece = product[:, i * head_dim:(i + 1) * head_dim].reshape(2, 2, half, head_dim)
                out_ref[pack * c + i, near_owner, :, :, :head_dim] = piece[0]
                out_ref[pack * c + i, far_owner, :, :, :head_dim] = piece[1]
            return carry

        lax.fori_loop(low, high, one, 0)

    load_own.wait()
    for t in range(2):
        to_far(buf.at[0, 2 + t], t).start()
    for t in range(2):
        to_near(buf.at[0, 2 + t], t).start()
    out_ref[...] = jnp.zeros_like(out_ref)
    for t in range(2):
        to_near(near_slot(t), t).wait_recv()
    load_w.wait()
    cut = [n_parts * i // 4 for i in range(5)]

    def step(k, carry):
        for h in range(2):
            t = 2 * k + h
            to_far(far_slot(t), t).wait_recv()
            to_near(far_slot(t), t + 2).start()
            multiply(k, cut[2 * h], cut[2 * h + 1])
            to_near(near_slot(t + 2), t + 2).wait_recv()

            @pl.when(t + 2 < n - 2)
            def _():
                to_far(near_slot(t + 2), t + 2).start()

            multiply(k, cut[2 * h + 1], cut[2 * h + 2])
        return carry

    lax.fori_loop(0, n // 2 - 1, step, 0)
    multiply(n // 2 - 1, 0, n_parts)

    def finish(t, carry):
        to_near(buf.at[0, 0], t).wait_send()
        return carry

    lax.fori_loop(0, n, finish, 0)

    def finish_far(t, carry):
        to_far(buf.at[0, 0], t).wait_send()
        return carry

    lax.fori_loop(0, n - 2, finish_far, 0)


def ring_qkv(normed, w, bias, n, pack):
    _, half, width = normed.shape
    dma = pltpu.SemaphoreType.DMA
    vmem = pl.BlockSpec(memory_space=pltpu.VMEM)
    return pl.pallas_call(
        functools.partial(ring_qkv_kernel, n, pack),
        out_shape=jax.ShapeDtypeStruct((pack * w.shape[0], n, 2, half, 128), BF16),
        in_specs=[pl.BlockSpec(memory_space=pl.ANY), pl.BlockSpec(memory_space=pl.ANY), vmem],
        out_specs=vmem,
        scratch_shapes=[
            pltpu.VMEM(w.shape, BF16),
            pltpu.VMEM((n // 2, 4, half, width), BF16),
            dma((2,)), dma((n - 2,)), dma((n,)), dma((n - 2,)), dma((n,)),
        ],
        compiler_params=pltpu.CompilerParams(collective_id=2, has_side_effects=True, vmem_limit_bytes=VMEM_LIMIT),
        name="ring_qkv",
    )(normed, w, bias)


def ring_out_kernel(n, slots, qkv_ref, w_hbm, embed_hbm, bias_ref, out_ref, w_ref, embed_ref, load_sem, init_f, add_n, add_f, buf_n, buf_f,
                    send_f, send_n, recv_f, recv_n, free_f, free_n):
    ring = Ring(n)
    heads, head_dim, width = w_ref.shape
    half = embed_ref.shape[1]
    seq_len = qkv_ref.shape[1]
    chunk = width // 4
    scale = head_dim ** -0.5
    load_w = pltpu.make_async_copy(w_hbm, w_ref, load_sem.at[0])
    load_w.start()
    load_embed = pltpu.make_async_copy(embed_hbm, embed_ref, load_sem.at[1])
    load_embed.start()

    def term(places):
        firsts = [pl.multiple_of((block * 2 + which) * half, half) for block, which, _ in places]
        key = lax.broadcasted_iota(jnp.int32, (half, seq_len), 1)
        row = lax.broadcasted_iota(jnp.int32, (half, seq_len), 0)
        visible = jnp.concatenate([key - row for _ in places], axis=0) <= jnp.concatenate(
            [jnp.full((half, 1), first, jnp.int32) for first in firsts], axis=0
        )
        contexts = []
        for h in range(heads):
            query = jnp.concatenate([qkv_ref[h, pl.ds(first, half), :] for first in firsts], axis=0)
            scores = lax.dot_general(query, qkv_ref[heads + h], (((1,), (1,)), ((), ())), preferred_element_type=F32) * scale
            scores = jnp.where(visible, scores, -jnp.inf)
            scores = jnp.exp(scores - jnp.max(scores, axis=-1, keepdims=True))
            probs = (scores / jnp.sum(scores, axis=-1, keepdims=True)).astype(BF16)
            context = jnp.dot(probs, qkv_ref[2 * heads + h], preferred_element_type=F32).astype(BF16)
            contexts.append(context[:, :head_dim])
        for c in range(width // chunk):
            columns = slice(c * chunk, (c + 1) * chunk)
            total = jnp.dot(contexts[0], w_ref[0, :, columns], preferred_element_type=F32)
            for h in range(1, heads):
                total += jnp.dot(contexts[h], w_ref[h, :, columns], preferred_element_type=F32)
            for i, (_, _, dst) in enumerate(places):
                dst[:, columns] = total[i * half:(i + 1) * half]

    def near_place(t, dst):
        return ring.near_block(lax.div(t, 2) + 1), lax.rem(t, 2), dst

    def far_place(t, dst):
        return ring.far_block(lax.div(t, 2) + 1), lax.rem(t, 2), dst

    def near_term(t, dst):
        term([near_place(t, dst)])

    def far_term(t, dst):
        term([far_place(t, dst)])

    def to_far(src, t):
        return remote(src, buf_f.at[lax.rem(t, slots)], send_f.at[t], recv_f.at[t], ring.far)

    def to_near(src, t):
        return remote(src, buf_n.at[lax.rem(t, slots)], send_n.at[t], recv_n.at[t], ring.near)

    def pass_far_on(t):
        slot = lax.rem(t, slots)
        to_far(buf_f.at[slot], t).wait_recv()
        buf_f[slot] = buf_f[slot] + add_f[...]

        @pl.when(t + 2 >= slots)
        def _():
            pl.semaphore_wait(free_n, 1)

        to_near(buf_f.at[slot], t + 2).start()

    def pass_near_on(t):
        slot = lax.rem(t, slots)
        to_near(buf_n.at[slot], t).wait_recv()
        buf_n[slot] = buf_n[slot] + add_n[...]

        @pl.when(t >= slots)
        def _():
            pl.semaphore_wait(free_f, 1)

        to_far(buf_n.at[slot], t).start()

    def finish_near(t):
        slot = t % slots
        to_near(buf_n.at[slot], t).wait_recv()
        out_ref[t % 2] = (embed_ref[t % 2].astype(F32) + (buf_n[slot] + add_n[...]) + bias_ref[...]).astype(BF16)

    ring.barrier()

    load_w.wait()

    def pair(t, dst):
        term([far_place(t, dst), near_place(t, add_n)])

    def begin(t, carry):
        pair(t, init_f.at[t])

        @pl.when(t < 2)
        def _():
            to_near(init_f.at[t], t).start()
            pass_near_on(t)

        return carry

    lax.fori_loop(0, 3, begin, 0)
    load_embed.wait()

    add_f[...] = init_f[2]

    def step(t, carry):
        pass_far_on(t)
        far_term(t + 3, add_f)
        pass_near_on(t + 2)
        near_term(t + 3, add_n)

        @pl.when(t + slots < n - 2)
        def _():
            to_near(init_f.at[0], t + 2).wait_send()
            pl.semaphore_signal(free_f, inc=1, device_id={"tp": ring.far}, device_id_type=MESH)

        @pl.when((t >= 1) & (t - 1 + slots < n))
        def _():
            to_far(init_f.at[0], t - 1).wait_send()
            pl.semaphore_signal(free_n, inc=1, device_id={"tp": ring.near}, device_id_type=MESH)

        return carry

    lax.fori_loop(0, n - 4, step, 0)
    pass_far_on(n - 4)
    far_term(n - 1, add_f)
    finish_near(n - 2)
    near_term(n - 1, add_n)
    pass_far_on(n - 3)
    finish_near(n - 1)

    for t in range(2):
        to_near(init_f.at[0], t).wait_send()

    def finish(t, carry):
        to_near(init_f.at[0], t).wait_send()
        return carry

    lax.fori_loop(n - slots, n, finish, 0)

    def finish_far(t, carry):
        to_far(init_f.at[0], t).wait_send()
        return carry

    lax.fori_loop(n - slots, n - 2, finish_far, 0)


def ring_out(qkv, w_out, embed, b_out, n):
    _, half, width = embed.shape
    slots = n // 2
    dma = pltpu.SemaphoreType.DMA
    vmem = pl.BlockSpec(memory_space=pltpu.VMEM)
    return pl.pallas_call(
        functools.partial(ring_out_kernel, n, slots),
        out_shape=jax.ShapeDtypeStruct((2, half, width), BF16),
        in_specs=[vmem, pl.BlockSpec(memory_space=pl.ANY), pl.BlockSpec(memory_space=pl.ANY), vmem],
        out_specs=vmem,
        scratch_shapes=[
            pltpu.VMEM(w_out.shape, BF16),
            pltpu.VMEM((2, half, width), BF16),
            dma((2,)),
            pltpu.VMEM((3, half, width), F32),
            pltpu.VMEM((half, width), F32),
            pltpu.VMEM((half, width), F32),
            pltpu.VMEM((slots, half, width), F32),
            pltpu.VMEM((slots, half, width), F32),
            dma((n - 2,)), dma((n,)), dma((n - 2,)), dma((n,)),
            pltpu.SemaphoreType.REGULAR, pltpu.SemaphoreType.REGULAR,
        ],
        compiler_params=pltpu.CompilerParams(collective_id=3, has_side_effects=True, vmem_limit_bytes=VMEM_LIMIT),
        name="ring_out",
    )(qkv, w_out, embed, b_out)


LIMIT = 16
GROUP = 8


def pick_kernel(want_ref, column_ref, table_ref, out_ref, fetched, sems):
    j = pl.program_id(0)

    def each(block, slot, act):
        def one(k, carry):
            row = want_ref[block * LIMIT + k]

            @pl.when(row >= 0)
            def _():
                start = pl.multiple_of(lax.div(row, GROUP) * GROUP, GROUP)
                act(pltpu.make_async_copy(
                    table_ref.at[pl.ds(start, GROUP), :],
                    fetched.at[slot, k],
                    sems.at[slot, k],
                ))

            return carry

        lax.fori_loop(0, LIMIT, one, 0)

    @pl.when(j == 0)
    def _():
        fetched[...] = jnp.zeros_like(fetched)
        each(0, 0, lambda copy: copy.start())

    @pl.when(j + 1 < pl.num_programs(0))
    def _():
        each(j + 1, lax.rem(j + 1, 2), lambda copy: copy.start())

    slot = lax.rem(j, 2)
    columns = lax.broadcasted_iota(jnp.int32, (LIMIT, LIMIT * GROUP), 1)
    place = lax.broadcasted_iota(jnp.int32, (LIMIT, LIMIT * GROUP), 0) * GROUP
    row = column_ref[...]
    selector = jnp.where((row >= 0) & (columns == place + lax.rem(jnp.maximum(row, 0), GROUP)), 1.0, 0.0).astype(BF16)
    each(j, slot, lambda copy: copy.wait())
    out_ref[...] = jnp.dot(selector, fetched[slot].reshape(LIMIT * GROUP, out_ref.shape[1]), preferred_element_type=F32).astype(BF16)


def pick_rows(want, table, n):
    width = table.shape[1]
    return pl.pallas_call(
        pick_kernel,
        grid=(n,),
        out_shape=jax.ShapeDtypeStruct((n * LIMIT, width), BF16),
        in_specs=[
            pl.BlockSpec(memory_space=pltpu.SMEM),
            pl.BlockSpec((LIMIT, 1), lambda j: (j, 0)),
            pl.BlockSpec(memory_space=pl.ANY),
        ],
        out_specs=pl.BlockSpec((LIMIT, width), lambda j: (j, 0)),
        scratch_shapes=[pltpu.VMEM((2, LIMIT, GROUP, width), BF16), pltpu.SemaphoreType.DMA((2, LIMIT))],
        compiler_params=pltpu.CompilerParams(vmem_limit_bytes=VMEM_LIMIT),
        name="pick_rows",
    )(want, want.reshape(n * LIMIT, 1), table)


def exchange_kernel(n, picked_ref, index_ref, out_ref, got, own_sem, send, recv):
    me = lax.axis_index("tp")
    own = pltpu.make_async_copy(picked_ref.at[me], got.at[me], own_sem.at[0])
    own.start()
    barrier = pltpu.get_barrier_semaphore()

    def greet(j, carry):
        pl.semaphore_signal(barrier, inc=1, device_id={"tp": lax.rem(me + j, n)}, device_id_type=MESH)
        return carry

    lax.fori_loop(1, n, greet, 0)
    pl.semaphore_wait(barrier, n - 1)

    def copy_to(j):
        other = lax.rem(me + j, n)
        return remote(picked_ref.at[other], got.at[me], send.at[j], recv.at[j], other)

    for j in range(n // 2, 0, -1):
        copy_to(j).start()
        if j < n // 2:
            copy_to(n - j).start()

    def arrive(j, carry):
        source = lax.rem(me - j + n, n)
        remote(picked_ref.at[0], got.at[source], send.at[j], recv.at[j], source).wait_recv()
        return carry

    lax.fori_loop(1, n, arrive, 0)
    own.wait()
    block_len, width = out_ref.shape
    rows = n * LIMIT
    selector = jnp.where(lax.broadcasted_iota(jnp.int32, (block_len, rows), 1) == index_ref[...], 1.0, 0.0).astype(BF16)
    chunk = width // 4
    for c in range(4):
        columns = slice(c * chunk, (c + 1) * chunk)
        out_ref[:, columns] = jnp.dot(
            selector, got[:, :, columns].reshape(rows, chunk), preferred_element_type=F32
        ).astype(BF16)

    def sent(j, carry):
        copy_to(j).wait_send()
        return carry

    lax.fori_loop(1, n, sent, 0)


def exchange(picked, index, n):
    _, _, width = picked.shape
    dma = pltpu.SemaphoreType.DMA
    vmem = pl.BlockSpec(memory_space=pltpu.VMEM)
    return pl.pallas_call(
        functools.partial(exchange_kernel, n),
        out_shape=jax.ShapeDtypeStruct((index.shape[0], width), BF16),
        in_specs=[pl.BlockSpec(memory_space=pl.ANY), vmem],
        out_specs=vmem,
        scratch_shapes=[pltpu.VMEM((n, LIMIT, width), BF16), dma((1,)), dma((n,)), dma((n,))],
        compiler_params=pltpu.CompilerParams(collective_id=4, has_side_effects=True, vmem_limit_bytes=VMEM_LIMIT),
        name="exchange",
    )(picked, index)


def look_up(token_ids, table, n):
    shard_rows, width = table.shape
    me = lax.axis_index("tp")
    ids = token_ids.reshape(n, -1)
    block_len = ids.shape[1]
    earlier = lax.broadcasted_iota(jnp.int32, (block_len, block_len), 0) > lax.broadcasted_iota(jnp.int32, (block_len, block_len), 1)
    same = ids[:, :, None] == ids[:, None, :]
    fresh = jnp.sum((same & earlier[None]).astype(jnp.int32), axis=2) == 0
    owner = lax.div(ids, shard_rows)
    rank = jnp.sum(((owner[:, :, None] == owner[:, None, :]) & earlier[None] & fresh[:, None, :]).astype(jnp.int32), axis=2)
    overflow = jnp.max(jnp.where(fresh, rank, 0)) >= LIMIT
    places = lax.broadcasted_iota(jnp.int32, (n, LIMIT, block_len), 1)
    wanted = (places == rank[:, None, :]) & (fresh & (owner == me))[:, None, :]
    want = jnp.sum(jnp.where(wanted, (ids - me * shard_rows)[:, None, :] + 1, 0), axis=2) - 1

    my_ids = lax.dynamic_index_in_dim(ids, me, 0, keepdims=False)
    my_slots = lax.dynamic_index_in_dim(jnp.where(fresh, owner * LIMIT + rank, 0), me, 0, keepdims=False)
    my_fresh = lax.dynamic_index_in_dim(fresh, me, 0, keepdims=False)
    match = (my_ids[:, None] == my_ids[None, :]) & my_fresh[None, :]
    index = jnp.sum(jnp.where(match, my_slots[None, :], 0), axis=1)

    def by_exchange():
        return exchange(pick_rows(want.reshape(n * LIMIT), table, n).reshape(n, LIMIT, width), index.reshape(block_len, 1), n)

    def by_sum():
        local_ids = token_ids.reshape(n * block_len) - me * shard_rows
        partial_rows = gather_rows(local_ids, table, block_len)
        return ring_sum(partial_rows.reshape(n, 2, block_len // 2, width), n).reshape(block_len, width)

    return lax.cond(overflow, by_sum, by_exchange)


def solution(mesh):
    n = mesh.shape["tp"]

    def local_step(token_ids, word_shard, pos_table, ln_gain, ln_bias, w_qkv, b_qkv, w_out, b_out):
        width = word_shard.shape[1]
        seq_len = token_ids.shape[1]
        block_len = seq_len // n
        half = block_len // 2
        heads, head_dim = w_qkv.shape[2:]
        tp_index = lax.axis_index("tp")

        pack = 2 if heads % 2 == 0 else 1
        w = jnp.transpose(w_qkv, (1, 2, 3, 0)).reshape(3 * heads // pack, pack * head_dim, width)
        bias = b_qkv.reshape(3 * heads // pack, 1, pack * head_dim)

        block_rows = look_up(token_ids.reshape(seq_len), word_shard, n)
        pos_block = lax.dynamic_slice_in_dim(pos_table, tp_index * block_len, block_len, axis=0)
        embed = (block_rows.astype(F32) + pos_block.astype(F32)).astype(BF16)
        normed = layer_norm(embed.astype(F32), ln_gain, ln_bias).astype(BF16)
        qkv = ring_qkv(normed.reshape(2, half, width), w, bias, n, pack)
        resid = ring_out(qkv.reshape(3 * heads, seq_len, 128), w_out, embed.reshape(2, half, width), b_out.reshape(1, width), n)
        return resid.reshape(1, block_len, width), embed.reshape(1, block_len, width)

    in_specs = (P("dp", None), P("tp", None), P(None, None), P(None), P(None), P(None, None, "tp", None), P(None, "tp", None), P("tp", None, None), P(None))
    out_specs = (P("dp", "tp", None), P("dp", "tp", None))
    return jax.shard_map(local_step, mesh=mesh, in_specs=in_specs, out_specs=out_specs, check_vma=False)
```

```python
import functools

import jax
import jax.numpy as jnp
from jax import lax
from jax.experimental import pallas as pl
from jax.experimental.pallas import tpu as pltpu
from jax.sharding import PartitionSpec as P

LN_EPS = 1e-5
MESH = pl.DeviceIdType.MESH
BF16 = jnp.bfloat16
F32 = jnp.float32
VMEM_LIMIT = 67043328


def layer_norm(values, gain, bias):
    feat_mean = jnp.mean(values, axis=-1, keepdims=True)
    centered = values - feat_mean
    feat_variance = jnp.mean(centered * centered, axis=-1, keepdims=True)
    return centered * lax.rsqrt(feat_variance + LN_EPS) * gain + bias


ROWS = 16
FETCHES = 16
NONE = -(2**30)


def gather_kernel(block_len, shard_rows, ids_ref, column_ref, table_ref, out_ref, found, count, stamp, fetched, sems):
    j = pl.program_id(0)
    n_blocks = pl.num_programs(0)
    n_groups = shard_rows // ROWS

    def scan(block):
        base = lax.rem(block, 2) * (2 * block_len)

        def one(q, total):
            local_id = ids_ref[block * block_len + q]
            mine = (local_id >= 0) & (local_id < shard_rows)
            group = jnp.where(mine, lax.div(local_id, ROWS), n_groups)
            fresh = mine & (stamp[group] != block)
            stamp[group] = block
            found[base + total] = group
            return total + jnp.where(fresh, 1, 0)

        count[lax.rem(block, 2)] = lax.fori_loop(0, block_len, one, 0, unroll=8)

    def copy_of(block, chunk, k, slot):
        group = found[lax.rem(block, 2) * (2 * block_len) + chunk * FETCHES + k]
        return pltpu.make_async_copy(
            table_ref.at[pl.ds(pl.multiple_of(group * ROWS, ROWS), ROWS), :],
            fetched.at[slot, pl.ds(pl.multiple_of(k * ROWS, ROWS), ROWS), :],
            sems.at[slot, k],
        )

    def in_chunk(block, chunk):
        return jnp.minimum(count[lax.rem(block, 2)] - chunk * FETCHES, FETCHES)

    def start(block, chunk, slot):
        def one(k, carry):
            copy_of(block, chunk, k, slot).start()
            return carry

        lax.fori_loop(0, in_chunk(block, chunk), one, 0)

    def wait(block, chunk, slot):
        def one(k, carry):
            copy_of(block, chunk, k, slot).wait()
            return carry

        lax.fori_loop(0, in_chunk(block, chunk), one, 0)

    def selector(block, chunk):
        columns = lax.broadcasted_iota(jnp.int32, (1, FETCHES * ROWS), 1)
        base = lax.rem(block, 2) * (2 * block_len) + chunk * FETCHES
        held = in_chunk(block, chunk)
        first = jnp.full((1, FETCHES * ROWS), NONE, jnp.int32)
        for k in range(FETCHES):
            first = jnp.where(lax.div(columns, ROWS) == k, jnp.where(k < held, found[base + k] * ROWS, NONE), first)
        return jnp.where(column_ref[...] == first + lax.rem(columns, ROWS), 1.0, 0.0).astype(BF16)

    @pl.when(j == 0)
    def _():
        fetched[...] = jnp.zeros_like(fetched)

        def clear(g, carry):
            stamp[g] = -1
            return carry

        lax.fori_loop(0, n_groups + 1, clear, 0)
        scan(0)
        start(0, 0, 0)

    @pl.when(j + 1 < n_blocks)
    def _():
        scan(j + 1)
        start(j + 1, 0, lax.rem(j + 1, 2))

    slot = lax.rem(j, 2)
    wait(j, 0, slot)
    out_ref[...] = jnp.dot(selector(j, 0), fetched[slot], preferred_element_type=F32).astype(BF16)

    def more(chunk, carry):
        start(j, chunk, slot)
        wait(j, chunk, slot)
        out_ref[...] += jnp.dot(selector(j, chunk), fetched[slot], preferred_element_type=F32).astype(BF16)
        return carry

    lax.fori_loop(1, lax.div(count[slot] + (FETCHES - 1), FETCHES), more, 0)


def gather_rows(local_ids, table, block_len):
    (n_ids,), (shard_rows, width) = local_ids.shape, table.shape
    return pl.pallas_call(
        functools.partial(gather_kernel, block_len, shard_rows),
        grid=(n_ids // block_len,),
        out_shape=jax.ShapeDtypeStruct((n_ids, width), BF16),
        in_specs=[
            pl.BlockSpec(memory_space=pltpu.SMEM),
            pl.BlockSpec((block_len, 1), lambda j: (j, 0)),
            pl.BlockSpec(memory_space=pl.ANY),
        ],
        out_specs=pl.BlockSpec((block_len, width), lambda j: (j, 0)),
        scratch_shapes=[
            pltpu.SMEM((4 * block_len,), jnp.int32),
            pltpu.SMEM((2,), jnp.int32),
            pltpu.SMEM((shard_rows // ROWS + 1,), jnp.int32),
            pltpu.VMEM((2, FETCHES * ROWS, width), BF16),
            pltpu.SemaphoreType.DMA((2, FETCHES)),
        ],
        compiler_params=pltpu.CompilerParams(vmem_limit_bytes=40 * 2**20),
        name="gather_rows",
    )(local_ids, local_ids.reshape(n_ids, 1), table)


class Ring:
    def __init__(self, n):
        self.chips = n // 2
        self.me = lax.axis_index("tp")
        self.odd = lax.rem(self.me, 2)
        self.chip = lax.div(self.me, 2)
        self.way = 2 * self.odd - 1
        self.near = self.me - self.way
        self.far = lax.rem(self.me + self.way + n, n)

    def near_block(self, k):
        return 2 * lax.rem(self.chip - self.way * k + 2 * self.chips, self.chips) + self.odd

    def far_block(self, k):
        return 2 * lax.rem(self.chip + self.way * k + 2 * self.chips, self.chips) + 1 - self.odd

    def barrier(self):
        sem = pltpu.get_barrier_semaphore()
        for device in (self.near, self.far):
            pl.semaphore_signal(sem, inc=1, device_id={"tp": device}, device_id_type=MESH)
        pl.semaphore_wait(sem, 2)


def remote(src, dst, send_sem, recv_sem, device):
    return pltpu.make_async_remote_copy(
        src_ref=src, dst_ref=dst, send_sem=send_sem, recv_sem=recv_sem, device_id={"tp": device}, device_id_type=MESH
    )


def ring_sum_kernel(n, part_ref, out_ref, own_n, own_f, buf_n, buf_f, own_sem, send_f, send_n, recv_f, recv_n):
    ring = Ring(n)

    def load_n(t):
        return pltpu.make_async_copy(part_ref.at[ring.near_block(lax.div(t, 2) + 1), lax.rem(t, 2)], own_n.at[t], own_sem.at[0, t])

    def load_f(t):
        return pltpu.make_async_copy(part_ref.at[ring.far_block(lax.div(t, 2) + 1), lax.rem(t, 2)], own_f.at[t], own_sem.at[1, t])

    def start_loads(t, carry):
        load_f(t).start()
        load_n(t).start()
        return carry

    lax.fori_loop(0, n, start_loads, 0)
    ring.barrier()

    def to_far(src, t):
        return remote(src, buf_f.at[t], send_f.at[t], recv_f.at[t], ring.far)

    def to_near(src, t):
        return remote(src, buf_n.at[t], send_n.at[t], recv_n.at[t], ring.near)

    def pass_far_on(t):
        to_far(buf_f.at[t], t).wait_recv()
        load_f(t + 2).wait()
        buf_f[t] = buf_f[t] + own_f[t + 2]
        to_near(buf_f.at[t], t + 2).start()

    def take_near(t):
        to_near(buf_n.at[t], t).wait_recv()
        load_n(t).wait()

    def pass_near_on(t):
        take_near(t)
        buf_n[t] = buf_n[t] + own_n[t]
        to_far(buf_n.at[t], t).start()

    def finish_near(t):
        take_near(t)
        out_ref[t % 2] = buf_n[t] + own_n[t]

    for t in range(2):
        load_f(t).wait()
        to_near(own_f.at[t], t).start()
    for t in range(2):
        pass_near_on(t)

    def step(t, carry):
        pass_far_on(t)
        pass_near_on(t + 2)
        return carry

    lax.fori_loop(0, n - 4, step, 0)
    for t in (n - 4, n - 3):
        pass_far_on(t)
        finish_near(t + 2)

    def finish(t, carry):
        to_near(own_f.at[t], t).wait_send()
        return carry

    lax.fori_loop(0, n, finish, 0)

    def finish_far(t, carry):
        to_far(buf_n.at[t], t).wait_send()
        return carry

    lax.fori_loop(0, n - 2, finish_far, 0)


def ring_sum(partial_rows, n):
    _, _, half, width = partial_rows.shape
    dma = pltpu.SemaphoreType.DMA
    return pl.pallas_call(
        functools.partial(ring_sum_kernel, n),
        out_shape=jax.ShapeDtypeStruct((2, half, width), BF16),
        in_specs=[pl.BlockSpec(memory_space=pl.ANY)],
        out_specs=pl.BlockSpec(memory_space=pltpu.VMEM),
        scratch_shapes=[
            pltpu.VMEM((n, half, width), BF16),
            pltpu.VMEM((n, half, width), BF16),
            pltpu.VMEM((n, half, width), BF16),
            pltpu.VMEM((n - 2, half, width), BF16),
            dma((2, n)), dma((n - 2,)), dma((n,)), dma((n - 2,)), dma((n,)),
        ],
        compiler_params=pltpu.CompilerParams(collective_id=1, has_side_effects=True, vmem_limit_bytes=VMEM_LIMIT),
        name="ring_sum",
    )(partial_rows)


def ring_qkv_kernel(n, pack, own_hbm, w_hbm, bias_ref, out_ref, w_ref, buf, load_sem, send_f, send_n, recv_f, recv_n):
    ring = Ring(n)
    _, _, half, width = buf.shape
    n_parts, part_width = w_ref.shape[:2]
    head_dim = part_width // pack
    load_own = pltpu.make_async_copy(own_hbm, buf.at[0, pl.ds(2, 2)], load_sem.at[0])
    load_own.start()
    load_w = pltpu.make_async_copy(w_hbm, w_ref, load_sem.at[1])
    load_w.start()
    ring.barrier()

    def near_slot(t):
        return buf.at[lax.div(t, 2), lax.rem(t, 2)]

    def far_slot(t):
        return buf.at[lax.div(t, 2) + 1, 2 + lax.rem(t, 2)]

    def to_far(src, t):
        return remote(src, far_slot(t), send_f.at[t], recv_f.at[t], ring.far)

    def to_near(src, t):
        return remote(src, near_slot(t), send_n.at[t], recv_n.at[t], ring.near)

    def multiply(k, low, high):
        near_owner = jnp.where(k == 0, ring.near, ring.near_block(k))
        far_owner = jnp.where(k == 0, ring.me, ring.far_block(k))

        def one(c, carry):
            product = lax.dot_general(
                buf[k].reshape(4 * half, width), w_ref[c], (((1,), (1,)), ((), ())), preferred_element_type=F32
            )
            product = (product + bias_ref[c]).astype(BF16)
            for i in range(pack):
                piece = product[:, i * head_dim:(i + 1) * head_dim].reshape(2, 2, half, head_dim)
                out_ref[pack * c + i, near_owner, :, :, :head_dim] = piece[0]
                out_ref[pack * c + i, far_owner, :, :, :head_dim] = piece[1]
            return carry

        lax.fori_loop(low, high, one, 0)

    load_own.wait()
    for t in range(2):
        to_far(buf.at[0, 2 + t], t).start()
    for t in range(2):
        to_near(buf.at[0, 2 + t], t).start()
    out_ref[...] = jnp.zeros_like(out_ref)
    for t in range(2):
        to_near(near_slot(t), t).wait_recv()
    load_w.wait()
    cut = [n_parts * i // 4 for i in range(5)]

    def step(k, carry):
        for h in range(2):
            t = 2 * k + h
            to_far(far_slot(t), t).wait_recv()
            to_near(far_slot(t), t + 2).start()
            multiply(k, cut[2 * h], cut[2 * h + 1])
            to_near(near_slot(t + 2), t + 2).wait_recv()

            @pl.when(t + 2 < n - 2)
            def _():
                to_far(near_slot(t + 2), t + 2).start()

            multiply(k, cut[2 * h + 1], cut[2 * h + 2])
        return carry

    lax.fori_loop(0, n // 2 - 1, step, 0)
    multiply(n // 2 - 1, 0, n_parts)

    def finish(t, carry):
        to_near(buf.at[0, 0], t).wait_send()
        return carry

    lax.fori_loop(0, n, finish, 0)

    def finish_far(t, carry):
        to_far(buf.at[0, 0], t).wait_send()
        return carry

    lax.fori_loop(0, n - 2, finish_far, 0)


def ring_qkv(normed, w, bias, n, pack):
    _, half, width = normed.shape
    dma = pltpu.SemaphoreType.DMA
    vmem = pl.BlockSpec(memory_space=pltpu.VMEM)
    return pl.pallas_call(
        functools.partial(ring_qkv_kernel, n, pack),
        out_shape=jax.ShapeDtypeStruct((pack * w.shape[0], n, 2, half, 128), BF16),
        in_specs=[pl.BlockSpec(memory_space=pl.ANY), pl.BlockSpec(memory_space=pl.ANY), vmem],
        out_specs=vmem,
        scratch_shapes=[
            pltpu.VMEM(w.shape, BF16),
            pltpu.VMEM((n // 2, 4, half, width), BF16),
            dma((2,)), dma((n - 2,)), dma((n,)), dma((n - 2,)), dma((n,)),
        ],
        compiler_params=pltpu.CompilerParams(collective_id=2, has_side_effects=True, vmem_limit_bytes=VMEM_LIMIT),
        name="ring_qkv",
    )(normed, w, bias)


def ring_out_kernel(n, slots, qkv_hbm, w_hbm, embed_hbm, bias_ref, out_ref, qkv_ref, w_ref, embed_ref, load_sem, init_f, add_n, add_f, buf_n, buf_f,
                    send_f, send_n, recv_f, recv_n, free_f, free_n):
    ring = Ring(n)
    heads, head_dim, width = w_ref.shape
    half = embed_ref.shape[1]
    seq_len = qkv_ref.shape[1]
    chunk = width // 4
    scale = head_dim ** -0.5
    load_qkv = pltpu.make_async_copy(qkv_hbm, qkv_ref, load_sem.at[2])
    load_qkv.start()
    load_w = pltpu.make_async_copy(w_hbm, w_ref, load_sem.at[0])
    load_w.start()
    load_embed = pltpu.make_async_copy(embed_hbm, embed_ref, load_sem.at[1])
    load_embed.start()

    def term(places):
        firsts = [pl.multiple_of((block * 2 + which) * half, half) for block, which, _ in places]
        key = lax.broadcasted_iota(jnp.int32, (half, seq_len), 1)
        row = lax.broadcasted_iota(jnp.int32, (half, seq_len), 0)
        visible = jnp.concatenate([key - row for _ in places], axis=0) <= jnp.concatenate(
            [jnp.full((half, 1), first, jnp.int32) for first in firsts], axis=0
        )
        contexts = []
        for h in range(heads):
            query = jnp.concatenate([qkv_ref[h, pl.ds(first, half), :] for first in firsts], axis=0)
            scores = lax.dot_general(query, qkv_ref[heads + h], (((1,), (1,)), ((), ())), preferred_element_type=F32) * scale
            scores = jnp.where(visible, scores, -jnp.inf)
            scores = jnp.exp(scores - jnp.max(scores, axis=-1, keepdims=True))
            probs = (scores / jnp.sum(scores, axis=-1, keepdims=True)).astype(BF16)
            context = jnp.dot(probs, qkv_ref[2 * heads + h], preferred_element_type=F32).astype(BF16)
            contexts.append(context[:, :head_dim])
        for c in range(width // chunk):
            columns = slice(c * chunk, (c + 1) * chunk)
            total = jnp.dot(contexts[0], w_ref[0, :, columns], preferred_element_type=F32)
            for h in range(1, heads):
                total += jnp.dot(contexts[h], w_ref[h, :, columns], preferred_element_type=F32)
            for i, (_, _, dst) in enumerate(places):
                dst[:, columns] = total[i * half:(i + 1) * half]

    def near_place(t, dst):
        return ring.near_block(lax.div(t, 2) + 1), lax.rem(t, 2), dst

    def far_place(t, dst):
        return ring.far_block(lax.div(t, 2) + 1), lax.rem(t, 2), dst

    def near_term(t, dst):
        term([near_place(t, dst)])

    def far_term(t, dst):
        term([far_place(t, dst)])

    def to_far(src, t):
        return remote(src, buf_f.at[lax.rem(t, slots)], send_f.at[t], recv_f.at[t], ring.far)

    def to_near(src, t):
        return remote(src, buf_n.at[lax.rem(t, slots)], send_n.at[t], recv_n.at[t], ring.near)

    def pass_far_on(t):
        slot = lax.rem(t, slots)
        to_far(buf_f.at[slot], t).wait_recv()
        buf_f[slot] = buf_f[slot] + add_f[...]

        @pl.when(t + 2 >= slots)
        def _():
            pl.semaphore_wait(free_n, 1)

        to_near(buf_f.at[slot], t + 2).start()

    def pass_near_on(t):
        slot = lax.rem(t, slots)
        to_near(buf_n.at[slot], t).wait_recv()
        buf_n[slot] = buf_n[slot] + add_n[...]

        @pl.when(t >= slots)
        def _():
            pl.semaphore_wait(free_f, 1)

        to_far(buf_n.at[slot], t).start()

    def finish_near(t):
        slot = t % slots
        to_near(buf_n.at[slot], t).wait_recv()
        out_ref[t % 2] = (embed_ref[t % 2].astype(F32) + (buf_n[slot] + add_n[...]) + bias_ref[...]).astype(BF16)

    ring.barrier()
    load_qkv.wait()
    load_w.wait()

    def pair(t, dst):
        term([far_place(t, dst), near_place(t, add_n)])

    def begin(t, carry):
        pair(t, init_f.at[t])

        @pl.when(t < 2)
        def _():
            to_near(init_f.at[t], t).start()
            pass_near_on(t)

        return carry

    lax.fori_loop(0, 3, begin, 0)
    load_embed.wait()

    add_f[...] = init_f[2]

    def step(t, carry):
        pass_far_on(t)
        far_term(t + 3, add_f)
        pass_near_on(t + 2)
        near_term(t + 3, add_n)

        @pl.when(t + slots < n - 2)
        def _():
            to_near(init_f.at[0], t + 2).wait_send()
            pl.semaphore_signal(free_f, inc=1, device_id={"tp": ring.far}, device_id_type=MESH)

        @pl.when((t >= 1) & (t - 1 + slots < n))
        def _():
            to_far(init_f.at[0], t - 1).wait_send()
            pl.semaphore_signal(free_n, inc=1, device_id={"tp": ring.near}, device_id_type=MESH)

        return carry

    lax.fori_loop(0, n - 4, step, 0)
    pass_far_on(n - 4)
    far_term(n - 1, add_f)
    finish_near(n - 2)
    near_term(n - 1, add_n)
    pass_far_on(n - 3)
    finish_near(n - 1)

    for t in range(2):
        to_near(init_f.at[0], t).wait_send()

    def finish(t, carry):
        to_near(init_f.at[0], t).wait_send()
        return carry

    lax.fori_loop(n - slots, n, finish, 0)

    def finish_far(t, carry):
        to_far(init_f.at[0], t).wait_send()
        return carry

    lax.fori_loop(n - slots, n - 2, finish_far, 0)


def ring_out(qkv, w_out, embed, b_out, n):
    _, half, width = embed.shape
    slots = n // 2
    dma = pltpu.SemaphoreType.DMA
    vmem = pl.BlockSpec(memory_space=pltpu.VMEM)
    return pl.pallas_call(
        functools.partial(ring_out_kernel, n, slots),
        out_shape=jax.ShapeDtypeStruct((2, half, width), BF16),
        in_specs=[pl.BlockSpec(memory_space=pl.ANY)] * 3 + [vmem],
        out_specs=vmem,
        scratch_shapes=[
            pltpu.VMEM(qkv.shape, BF16),
            pltpu.VMEM(w_out.shape, BF16),
            pltpu.VMEM((2, half, width), BF16),
            dma((3,)),
            pltpu.VMEM((3, half, width), F32),
            pltpu.VMEM((half, width), F32),
            pltpu.VMEM((half, width), F32),
            pltpu.VMEM((slots, half, width), F32),
            pltpu.VMEM((slots, half, width), F32),
            dma((n - 2,)), dma((n,)), dma((n - 2,)), dma((n,)),
            pltpu.SemaphoreType.REGULAR, pltpu.SemaphoreType.REGULAR,
        ],
        compiler_params=pltpu.CompilerParams(collective_id=3, has_side_effects=True, vmem_limit_bytes=VMEM_LIMIT),
        name="ring_out",
    )(qkv, w_out, embed, b_out)


LIMIT = 16
GROUP = 8
DEPTH = 4


def pick_kernel(want_ref, column_ref, table_ref, out_ref, fetched, sems):
    j = pl.program_id(0)

    def each(block, slot, act):
        def one(k, carry):
            row = want_ref[block * LIMIT + k]

            @pl.when(row >= 0)
            def _():
                start = pl.multiple_of(lax.div(row, GROUP) * GROUP, GROUP)
                act(pltpu.make_async_copy(
                    table_ref.at[pl.ds(start, GROUP), :],
                    fetched.at[slot, k],
                    sems.at[slot, k],
                ))

            return carry

        lax.fori_loop(0, LIMIT, one, 0)

    @pl.when(j == 0)
    def _():
        fetched[...] = jnp.zeros_like(fetched)
        for ahead in range(DEPTH - 1):
            each(ahead, ahead, lambda copy: copy.start())

    @pl.when(j + DEPTH - 1 < pl.num_programs(0))
    def _():
        each(j + DEPTH - 1, lax.rem(j + DEPTH - 1, DEPTH), lambda copy: copy.start())

    slot = lax.rem(j, DEPTH)
    columns = lax.broadcasted_iota(jnp.int32, (LIMIT, LIMIT * GROUP), 1)
    place = lax.broadcasted_iota(jnp.int32, (LIMIT, LIMIT * GROUP), 0) * GROUP
    row = column_ref[...]
    selector = jnp.where((row >= 0) & (columns == place + lax.rem(jnp.maximum(row, 0), GROUP)), 1.0, 0.0).astype(BF16)
    each(j, slot, lambda copy: copy.wait())
    out_ref[...] = jnp.dot(selector, fetched[slot].reshape(LIMIT * GROUP, out_ref.shape[1]), preferred_element_type=F32).astype(BF16)


def pick_rows(want, table, n):
    width = table.shape[1]
    return pl.pallas_call(
        pick_kernel,
        grid=(n,),
        out_shape=jax.ShapeDtypeStruct((n * LIMIT, width), BF16),
        in_specs=[
            pl.BlockSpec(memory_space=pltpu.SMEM),
            pl.BlockSpec((LIMIT, 1), lambda j: (j, 0)),
            pl.BlockSpec(memory_space=pl.ANY),
        ],
        out_specs=pl.BlockSpec((LIMIT, width), lambda j: (j, 0)),
        scratch_shapes=[pltpu.VMEM((DEPTH, LIMIT, GROUP, width), BF16), pltpu.SemaphoreType.DMA((DEPTH, LIMIT))],
        compiler_params=pltpu.CompilerParams(vmem_limit_bytes=VMEM_LIMIT),
        name="pick_rows",
    )(want, want.reshape(n * LIMIT, 1), table)


def exchange_kernel(n, picked_ref, index_ref, out_ref, got, own_sem, send, recv):
    me = lax.axis_index("tp")
    own = pltpu.make_async_copy(picked_ref.at[me], got.at[me], own_sem.at[0])
    own.start()
    barrier = pltpu.get_barrier_semaphore()

    def greet(j, carry):
        pl.semaphore_signal(barrier, inc=1, device_id={"tp": lax.rem(me + j, n)}, device_id_type=MESH)
        return carry

    lax.fori_loop(1, n, greet, 0)
    pl.semaphore_wait(barrier, n - 1)

    def copy_to(j):
        other = lax.rem(me + j, n)
        return remote(picked_ref.at[other], got.at[me], send.at[j], recv.at[j], other)

    for j in range(n // 2, 0, -1):
        copy_to(j).start()
        if j < n // 2:
            copy_to(n - j).start()

    def arrive(j, carry):
        source = lax.rem(me - j + n, n)
        remote(picked_ref.at[0], got.at[source], send.at[j], recv.at[j], source).wait_recv()
        return carry

    lax.fori_loop(1, n, arrive, 0)
    own.wait()
    block_len, width = out_ref.shape
    rows = n * LIMIT
    selector = jnp.where(lax.broadcasted_iota(jnp.int32, (block_len, rows), 1) == index_ref[...], 1.0, 0.0).astype(BF16)
    chunk = width // 4
    for c in range(4):
        columns = slice(c * chunk, (c + 1) * chunk)
        out_ref[:, columns] = jnp.dot(
            selector, got[:, :, columns].reshape(rows, chunk), preferred_element_type=F32
        ).astype(BF16)

    def sent(j, carry):
        copy_to(j).wait_send()
        return carry

    lax.fori_loop(1, n, sent, 0)


def exchange(picked, index, n):
    _, _, width = picked.shape
    dma = pltpu.SemaphoreType.DMA
    vmem = pl.BlockSpec(memory_space=pltpu.VMEM)
    return pl.pallas_call(
        functools.partial(exchange_kernel, n),
        out_shape=jax.ShapeDtypeStruct((index.shape[0], width), BF16),
        in_specs=[pl.BlockSpec(memory_space=pl.ANY), vmem],
        out_specs=vmem,
        scratch_shapes=[pltpu.VMEM((n, LIMIT, width), BF16), dma((1,)), dma((n,)), dma((n,))],
        compiler_params=pltpu.CompilerParams(collective_id=4, has_side_effects=True, vmem_limit_bytes=VMEM_LIMIT),
        name="exchange",
    )(picked, index)


def look_up(token_ids, table, n):
    shard_rows, width = table.shape
    me = lax.axis_index("tp")
    ids = token_ids.reshape(n, -1)
    block_len = ids.shape[1]
    earlier = lax.broadcasted_iota(jnp.int32, (block_len, block_len), 0) > lax.broadcasted_iota(jnp.int32, (block_len, block_len), 1)
    same = ids[:, :, None] == ids[:, None, :]
    fresh = jnp.sum((same & earlier[None]).astype(jnp.int32), axis=2) == 0
    owner = lax.div(ids, shard_rows)
    rank = jnp.sum(((owner[:, :, None] == owner[:, None, :]) & earlier[None] & fresh[:, None, :]).astype(jnp.int32), axis=2)
    overflow = jnp.max(jnp.where(fresh, rank, 0)) >= LIMIT
    places = lax.broadcasted_iota(jnp.int32, (n, LIMIT, block_len), 1)
    wanted = (places == rank[:, None, :]) & (fresh & (owner == me))[:, None, :]
    want = jnp.sum(jnp.where(wanted, (ids - me * shard_rows)[:, None, :] + 1, 0), axis=2) - 1

    my_ids = lax.dynamic_index_in_dim(ids, me, 0, keepdims=False)
    my_slots = lax.dynamic_index_in_dim(jnp.where(fresh, owner * LIMIT + rank, 0), me, 0, keepdims=False)
    my_fresh = lax.dynamic_index_in_dim(fresh, me, 0, keepdims=False)
    match = (my_ids[:, None] == my_ids[None, :]) & my_fresh[None, :]
    index = jnp.sum(jnp.where(match, my_slots[None, :], 0), axis=1)

    def by_exchange():
        return exchange(pick_rows(want.reshape(n * LIMIT), table, n).reshape(n, LIMIT, width), index.reshape(block_len, 1), n)

    def by_sum():
        local_ids = token_ids.reshape(n * block_len) - me * shard_rows
        partial_rows = gather_rows(local_ids, table, block_len)
        return ring_sum(partial_rows.reshape(n, 2, block_len // 2, width), n).reshape(block_len, width)

    return lax.cond(overflow, by_sum, by_exchange)


def solution(mesh):
    n = mesh.shape["tp"]

    def local_step(token_ids, word_shard, pos_table, ln_gain, ln_bias, w_qkv, b_qkv, w_out, b_out):
        width = word_shard.shape[1]
        seq_len = token_ids.shape[1]
        block_len = seq_len // n
        half = block_len // 2
        heads, head_dim = w_qkv.shape[2:]
        tp_index = lax.axis_index("tp")

        pack = 2 if heads % 2 == 0 else 1
        w = jnp.transpose(w_qkv, (1, 2, 3, 0)).reshape(3 * heads // pack, pack * head_dim, width)
        bias = b_qkv.reshape(3 * heads // pack, 1, pack * head_dim)

        block_rows = look_up(token_ids.reshape(seq_len), word_shard, n)
        pos_block = lax.dynamic_slice_in_dim(pos_table, tp_index * block_len, block_len, axis=0)
        embed = (block_rows.astype(F32) + pos_block.astype(F32)).astype(BF16)
        normed = layer_norm(embed.astype(F32), ln_gain, ln_bias).astype(BF16)
        qkv = ring_qkv(normed.reshape(2, half, width), w, bias, n, pack)
        resid = ring_out(qkv.reshape(3 * heads, seq_len, 128), w_out, embed.reshape(2, half, width), b_out.reshape(1, width), n)
        return resid.reshape(1, block_len, width), embed.reshape(1, block_len, width)

    in_specs = (P("dp", None), P("tp", None), P(None, None), P(None), P(None), P(None, None, "tp", None), P(None, "tp", None), P("tp", None, None), P(None))
    out_specs = (P("dp", "tp", None), P("dp", "tp", None))
    return jax.shard_map(local_step, mesh=mesh, in_specs=in_specs, out_specs=out_specs, check_vma=False)
```
